8 devices in a mesh: dp: 2 (over z, y), tp: 4 (over x, core).
Axes of the slice: x: 2, y: 2, z: 1, core: 2. Of those that a mesh axis runs over, the one named last changes fastest.
Arguments:
- tokens: bfloat16 [512, 512], P('dp'), parts along dimension 0
- seq_lens: int32 [512], P('dp'), parts along dimension 0
- k_cache: bfloat16 [2, 512, 76, 8, 64], P(None, 'dp', None, 'tp'), parts along dimension 1
- v_cache: bfloat16 [2, 512, 76, 8, 64], P(None, 'dp', None, 'tp'), parts along dimension 1
- mem_k: bfloat16 [2, 512, 256, 8, 64], P(None, 'dp', None, 'tp'), parts along dimension 1
- mem_v: bfloat16 [2, 512, 256, 8, 64], P(None, 'dp', None, 'tp'), parts along dimension 1
- ln_attn: float32 [2, 2, 512], replicated
- w_qkv: bfloat16 [2, 512, 3, 512], P(None, None, None, 'tp')
- b_qkv: float32 [2, 3, 512], P(None, None, 'tp')
- w_o: bfloat16 [2, 512, 512], P(None, 'tp')
- b_o: float32 [2, 512], replicated
- ln_cross: float32 [2, 2, 512], replicated
- w_qc: bfloat16 [2, 512, 512], P(None, None, 'tp')
- b_qc: float32 [2, 512], P(None, 'tp')
- w_oc: bfloat16 [2, 512, 512], P(None, 'tp')
- b_oc: float32 [2, 512], replicated
- ln_mlp: float32 [2, 2, 512], replicated
- w_fc1: bfloat16 [2, 512, 2048], P(None, None, 'tp')
- b_fc1: float32 [2, 2048], P(None, 'tp')
- w_fc2: bfloat16 [2, 2048, 512], P(None, 'tp')
- b_fc2: float32 [2, 512], replicated
- ln_final: float32 [2, 512], replicated
- w_out: bfloat16 [512, 49408], P(None, 'tp')
Outputs:
- output 1: float32 [512, 49408], P('dp', 'tp'), parts along dimension 0
- output 2: bfloat16 [2, 512, 76, 8, 64], P(None, 'dp', None, 'tp'), parts along dimension 1
- output 3: bfloat16 [2, 512, 76, 8, 64], P(None, 'dp', None, 'tp'), parts along dimension 1
There are 2 independent parts. The reference program is written for one: setup_inputs(seed, part) draws one part's arguments, and reference() takes and returns one part's arrays. A program takes and returns all parts, laid end to end along the dimension named above; an argument that names none is the same for every part.
All inputs are finite; a program needn't handle non-finite values.
Results may differ from the reference program's by a relative error of at most 0.00401784.
Values are sent between devices in bfloat16 or wider.
A program may use at most 1 GiB of HBM per device.

```python
import jax
import jax.numpy as jnp
from jax import lax

LAYERS = 2
BATCH_SEQS = 256
CONTEXT = 76
QUERIES = 256
MODEL_WIDTH = 512
NUM_HEADS = 8
HEAD_DIM = 64
FF_WIDTH = 2048
VOCAB_SIZE = 49408


def setup_inputs(seed: int = 0, part: int = 0) -> dict:
    part_keys = jax.random.split(jax.random.fold_in(jax.random.key(seed), part), 8)
    weight_keys = jax.random.split(jax.random.key(seed + 1), 20)
    cache_shape = (LAYERS, BATCH_SEQS, CONTEXT, NUM_HEADS, HEAD_DIM)
    memory_shape = (LAYERS, BATCH_SEQS, QUERIES, NUM_HEADS, HEAD_DIM)
    width_scale = MODEL_WIDTH ** -0.5
    ff_scale = FF_WIDTH ** -0.5

    def normal(key_index, shape, factor):
        return jax.random.normal(weight_keys[key_index], shape, jnp.float32) * factor

    def norm_params(key_index, shape):
        return normal(key_index, shape, 0.2) + jnp.array([1.0, 0.0], jnp.float32)[:, None]

    def part_normal(key_index, shape):
        return jax.random.normal(part_keys[key_index], shape, jnp.float32).astype(jnp.bfloat16)

    raw_lens = jax.random.randint(part_keys[1], (BATCH_SEQS,), 0, CONTEXT)
    full_row = jax.random.randint(part_keys[2], (), 0, BATCH_SEQS)
    seq_lens = jnp.where(jnp.arange(BATCH_SEQS) == full_row, CONTEXT - 1, raw_lens).astype(jnp.int32)
    return {
        'tokens': part_normal(0, (BATCH_SEQS, MODEL_WIDTH)),
        'seq_lens': seq_lens,
        'k_cache': part_normal(3, cache_shape),
        'v_cache': part_normal(4, cache_shape),
        'mem_k': part_normal(5, memory_shape),
        'mem_v': part_normal(6, memory_shape),
        'ln_attn': norm_params(0, (LAYERS, 2, MODEL_WIDTH)),
        'w_qkv': normal(1, (LAYERS, MODEL_WIDTH, 3, MODEL_WIDTH), width_scale).astype(jnp.bfloat16),
        'b_qkv': normal(2, (LAYERS, 3, MODEL_WIDTH), 0.5),
        'w_o': normal(3, (LAYERS, MODEL_WIDTH, MODEL_WIDTH), 3.0 * width_scale).astype(jnp.bfloat16),
        'b_o': normal(4, (LAYERS, MODEL_WIDTH), 0.3),
        'ln_cross': norm_params(5, (LAYERS, 2, MODEL_WIDTH)),
        'w_qc': normal(6, (LAYERS, MODEL_WIDTH, MODEL_WIDTH), 2.0 * width_scale).astype(jnp.bfloat16),
        'b_qc': normal(7, (LAYERS, MODEL_WIDTH), 1.0),
        'w_oc': normal(8, (LAYERS, MODEL_WIDTH, MODEL_WIDTH), 2.0 * width_scale).astype(jnp.bfloat16),
        'b_oc': normal(9, (LAYERS, MODEL_WIDTH), 0.3),
        'ln_mlp': norm_params(10, (LAYERS, 2, MODEL_WIDTH)),
        'w_fc1': normal(11, (LAYERS, MODEL_WIDTH, FF_WIDTH), width_scale).astype(jnp.bfloat16),
        'b_fc1': normal(12, (LAYERS, FF_WIDTH), 0.5),
        'w_fc2': normal(13, (LAYERS, FF_WIDTH, MODEL_WIDTH), 2.0 * ff_scale).astype(jnp.bfloat16),
        'b_fc2': normal(14, (LAYERS, MODEL_WIDTH), 0.3),
        'ln_final': norm_params(15, (2, MODEL_WIDTH)),
        'w_out': normal(16, (MODEL_WIDTH, VOCAB_SIZE), 3.0 * width_scale).astype(jnp.bfloat16),
    }


def layer_norm(hidden, params):
    mean_val = jnp.mean(hidden, axis=-1, keepdims=True)
    centred = hidden - mean_val
    variance = jnp.mean(centred * centred, axis=-1, keepdims=True)
    return (centred * lax.rsqrt(variance + 1e-5) * params[0] + params[1]).astype(jnp.bfloat16)


def attend(query_heads, key_heads, value_heads, keep_mask):
    scores = jnp.einsum('bhd,bjhd->bhj', query_heads.astype(jnp.float32), key_heads.astype(jnp.float32)) * (HEAD_DIM ** -0.5)
    scores = jnp.where(keep_mask, scores, -1e30)
    attn_probs = jax.nn.softmax(scores, axis=-1).astype(jnp.bfloat16)
    mixed_vals = jnp.einsum('bhj,bjhd->bhd', attn_probs.astype(jnp.float32), value_heads.astype(jnp.float32))
    return mixed_vals.astype(jnp.bfloat16).reshape(BATCH_SEQS, MODEL_WIDTH)


def reference(tokens, seq_lens, k_cache, v_cache, mem_k, mem_v, ln_attn, w_qkv, b_qkv, w_o, b_o, ln_cross, w_qc, b_qc, w_oc, b_oc, ln_mlp, w_fc1, b_fc1, w_fc2, b_fc2, ln_final, w_out):
    positions = jnp.arange(CONTEXT)
    write_mask = (positions[None, :] == seq_lens[:, None])[:, :, None, None]
    valid_mask = (positions[None, :] <= seq_lens[:, None])[:, None, :]
    layer_args = (k_cache, v_cache, mem_k, mem_v, ln_attn, w_qkv, b_qkv, w_o, b_o, ln_cross, w_qc, b_qc, w_oc, b_oc, ln_mlp, w_fc1, b_fc1, w_fc2, b_fc2)

    def layer_step(residual, params):
        (k_cache, v_cache, mem_k, mem_v, ln_attn, w_qkv, b_qkv, w_o, b_o, ln_cross, w_qc, b_qc, w_oc, b_oc, ln_mlp, w_fc1, b_fc1, w_fc2, b_fc2) = params
        normed = layer_norm(residual, ln_attn)
        qkv_vals = jnp.dot(normed, w_qkv.reshape(MODEL_WIDTH, 3 * MODEL_WIDTH), preferred_element_type=jnp.float32)
        qkv_heads = (qkv_vals.reshape(BATCH_SEQS, 3, MODEL_WIDTH) + b_qkv).astype(jnp.bfloat16).reshape(BATCH_SEQS, 3, NUM_HEADS, HEAD_DIM)
        key_cache = jnp.where(write_mask, qkv_heads[:, 1][:, None], k_cache)
        value_cache = jnp.where(write_mask, qkv_heads[:, 2][:, None], v_cache)
        attn_out = attend(qkv_heads[:, 0], key_cache, value_cache, valid_mask)
        residual = residual + jnp.dot(attn_out, w_o, preferred_element_type=jnp.float32) + b_o
        normed = layer_norm(residual, ln_cross)
        cross_query = (jnp.dot(normed, w_qc, preferred_element_type=jnp.float32) + b_qc).astype(jnp.bfloat16).reshape(BATCH_SEQS, NUM_HEADS, HEAD_DIM)
        cross_out = attend(cross_query, mem_k, mem_v, True)
        residual = residual + jnp.dot(cross_out, w_oc, preferred_element_type=jnp.float32) + b_oc
        normed = layer_norm(residual, ln_mlp)
        hidden = jax.nn.gelu(jnp.dot(normed, w_fc1, preferred_element_type=jnp.float32) + b_fc1, approximate=False).astype(jnp.bfloat16)
        residual = residual + jnp.dot(hidden, w_fc2, preferred_element_type=jnp.float32) + b_fc2
        return residual, (key_cache, value_cache)

    residual, (k_out, v_out) = lax.scan(layer_step, tokens.astype(jnp.float32), layer_args)
    logits = jnp.dot(layer_norm(residual, ln_final), w_out, preferred_element_type=jnp.float32)
    return jax.nn.log_softmax(logits, axis=-1), k_out, v_out
```

```python
import functools
import math

import jax
import jax.numpy as jnp
from jax import lax
from jax.experimental import pallas as pl
from jax.experimental.pallas import tpu as pltpu
from jax.sharding import PartitionSpec as P

BF = jnp.bfloat16
F32 = jnp.float32
MESH = pl.DeviceIdType.MESH
RING = 12
CHUNK = 16
HEAD_CHUNKS = 4
LANES = 128
HD = 64
ROWS = 256
WIDTH = 512


def dot(a, b):
    return jnp.dot(a, b, preferred_element_type=F32)


def dot_nt(a, b):
    return lax.dot_general(a, b, (((1,), (1,)), ((), ())), preferred_element_type=F32)


def norm(x, gain, shift):
    mean = jnp.mean(x, axis=-1, keepdims=True)
    centred = x - mean
    var = jnp.mean(centred * centred, axis=-1, keepdims=True)
    return (centred * lax.rsqrt(var + 1e-5) * gain + shift).astype(BF)


def fold(x8, op):
    x8 = op(x8, pltpu.roll(x8, 4, 0))
    return op(x8, pltpu.roll(x8, 2, 0))


def decode_kernel(tok, lens, kc, vc, mk, mv, lna, wqkv, bqkv, wo, bo, lnc, wqc, bqc, woc, boc, lnm, w1, b1, w2, b2, lnf, wout,
                  xn_out, lse_out, kn_out, vn_out,
                  mkb, mvb, ckb, cvb, wqkvb, wob, wqcb, w1b, w2b, woutb, b1x,
                  xown, xn0, xng, obuf, orecv, xsend, xrecv, q2s, qbm, pm, racc, qT, kT, vT, ss, msb, msr,
                  lw_sem, rws_sem, rwr_sem, c_sem, mk_sem, mv_sem, wo_sem, es, er, xs, xr, gs, gr, ls, lr):
    L = kc.shape[0]
    ctx = kc.shape[1]
    me = lax.axis_index('tp')
    c = lax.rem(me, 2)
    partner = me + 1 - 2 * c
    peer = lax.rem(me + 2, 4)
    own = pl.multiple_of(c * HD, HD)
    oth = pl.multiple_of((1 - c) * HD, HD)

    def seq_chunk(n):
        layer = n // 16
        within = n % 16
        half = within // 8
        sub = (within % 8) // 4
        grp = sub + (1 - 2 * sub) * (1 - c)
        seq = half * LANES + grp * HD + (within % 4) * CHUNK
        return layer, seq

    def mem_copies(n):
        layer, seq = seq_chunk(n)
        slot = n % RING
        return (pltpu.make_async_copy(mk.at[layer, pl.ds(seq, CHUNK)], mkb.at[slot], mk_sem.at[slot]),
                pltpu.make_async_copy(mv.at[layer, pl.ds(seq, CHUNK)], mvb.at[slot], mv_sem.at[slot]))

    def cache_copies(l):
        return (pltpu.make_async_copy(kc.at[l], ckb, c_sem.at[0]),
                pltpu.make_async_copy(vc.at[l], cvb, c_sem.at[1]))

    def weight_copies(l):
        pairs = ((wqkv.at[l], wqkvb.at[l]), (wo.at[l], wob.at[l, 0, 0]), (wqc.at[l], wqcb.at[l]),
                 (woc.at[l], wob.at[l, 1, 0]), (w1.at[l], w1b.at[l, 0]), (w2.at[l], w2b.at[l, 0]))
        return [pltpu.make_async_copy(s, d, lw_sem.at[l, i]) for i, (s, d) in enumerate(pairs)]

    def shared_copies(l):
        pairs = [(wo.at[l], wob.at[l, 0, 1]), (woc.at[l], wob.at[l, 1, 1]), (w1.at[l], w1b.at[l, 1]), (w2.at[l], w2b.at[l, 1])]
        if l == 0:
            pairs.append((b1, b1x))
        return [pltpu.make_async_remote_copy(s, d, rws_sem.at[l, i], rwr_sem.at[l, i], device_id={'tp': partner}, device_id_type=MESH)
                for i, (s, d) in enumerate(pairs)]

    def head_copies():
        rows = woutb.shape[1]
        return [pltpu.make_async_copy(wout.at[pl.ds(i * rows, rows)], woutb.at[i], wo_sem.at[i]) for i in range(HEAD_CHUNKS)]

    weights = [weight_copies(l) for l in range(L)]
    shared = [shared_copies(l) for l in range(L)]
    caches = [cache_copies(l) for l in range(L)]
    heads = head_copies()

    weights[0][0].start()
    caches[0][0].start()
    caches[0][1].start()
    for w in weights[0][1:]:
        w.start()
    for n in range(RING):
        for m in mem_copies(n):
            m.start()

    barrier = pltpu.get_barrier_semaphore()
    for d in range(1, 4):
        pl.semaphore_signal(barrier, inc=1, device_id={'tp': lax.rem(me + d, 4)}, device_id_type=MESH)
    pl.semaphore_wait(barrier, 3)
    for l in range(L):
        for s in shared[l]:
            s.start()
    for w in weights[1]:
        w.start()

    row = lax.broadcasted_iota(jnp.int32, (32, 2048), 0)
    lane = lax.broadcasted_iota(jnp.int32, (32, 2048), 1)
    qbm[...] = jnp.where(lane // HD == row, 1.0, 0.0).astype(BF)
    pm[...] = jnp.zeros_like(pm)
    for h in range(2):
        xown[h] = tok[pl.ds(pl.multiple_of(h * LANES + own, HD), HD), :].astype(F32)

    def self_attention(l, hf):
        lanes = pl.ds(hf * LANES, LANES)
        if l == 0:
            xn = norm(tok[hf * LANES:(hf + 1) * LANES, :].astype(F32), lna[0, 0:1], lna[0, 1:2])
            if hf == 0:
                weights[0][0].wait()
        else:
            if hf == 0:
                weights[1][0].wait()
            gathers[(l - 1, 1, hf)].wait()
            xn = xng[l - 1, 1, hf]
        for i, ref in enumerate((qT, kT, vT)):
            y = (dot(xn, wqkvb[l, i]) + bqkv[i, l:l + 1]).astype(BF)
            ref[...] = y.astype(F32).T
        kn_out[l, :, lanes] = kT[...].astype(BF)
        vn_out[l, :, lanes] = vT[...].astype(BF)
        if hf == 0:
            caches[l][0].wait()

        def k_body(t, _):
            blk = ckb[pl.ds(t * 4, 4), :, lanes].astype(F32) * qT[...][None]
            ss[pl.ds(pl.multiple_of(t * 8, 8), 8), :] = jnp.sum(blk.reshape(8, HD, LANES), axis=1) * 0.125
            return 0

        lax.fori_loop(0, ctx // 4, k_body, 0)
        snew = jnp.sum((qT[...] * kT[...]).reshape(2, HD, LANES), axis=1) * 0.125
        snew = jnp.concatenate([snew] * 4, axis=0)
        s = ss[...].reshape(ctx // 4, 8, LANES)
        pos = (lax.broadcasted_iota(jnp.int32, s.shape, 0) * 4 + lax.broadcasted_iota(jnp.int32, s.shape, 1) // 2)
        ln = lens[0:1, lanes][None]
        fresh = pos == ln
        s = jnp.where(fresh, snew[None], jnp.where(pos < ln, s, -1e30))
        m8 = fold(jnp.max(s, axis=0), jnp.maximum)
        p = jnp.exp(s - m8[None])
        l8 = fold(jnp.sum(p, axis=0), jnp.add)
        p = (p / l8[None]).astype(BF).astype(F32)
        pn = fold(jnp.sum(jnp.where(fresh, p, 0.0), axis=0), jnp.add)
        ss[...] = jnp.where(fresh, 0.0, p).reshape(ctx * 2, LANES)
        if hf == 0:
            caches[l][1].wait()

        def v_body(t, acc):
            blk = cvb[pl.ds(t * 4, 4), :, lanes].astype(F32)
            pr = ss[pl.ds(pl.multiple_of(t * 8, 8), 8), :]
            acc = list(acc)
            for j in range(4):
                for h in range(2):
                    acc[h] = acc[h] + blk[j, h * HD:(h + 1) * HD] * pr[2 * j + h:2 * j + h + 1]
            return tuple(acc)

        acc = tuple(vT[h * HD:(h + 1) * HD, :] * pn[h:h + 1] for h in range(2))
        acc = lax.fori_loop(0, ctx // 4, v_body, acc)
        oT = jnp.concatenate(acc, axis=0).astype(BF).astype(F32)
        obuf[l, 0, hf] = oT.T.astype(BF)
        send_o(l, 0, hf)

    sent = []
    swaps, crosses, gathers = {}, {}, {}

    def remote(src, dst, ssem, rsem, dev):
        cp = pltpu.make_async_remote_copy(src, dst, ssem, rsem, device_id={'tp': dev}, device_id_type=MESH)
        cp.start()
        return cp

    def send_o(l, k, hf):
        swaps[(l, k, hf)] = remote(obuf.at[l, k, hf, pl.ds(oth, HD)], orecv.at[l, k, hf], es.at[l, k, hf], er.at[l, k, hf], partner)

    def send_x(l, k, hf, part):
        xsend[l, k, hf] = part.astype(BF)
        crosses[(l, k, hf)] = remote(xsend.at[l, k, hf], xrecv.at[l, k, hf], xs.at[l, k, hf], xr.at[l, k, hf], peer)

    def project(l, k, hf):
        if hf == 0:
            weights[l][1 if k == 0 else 3].wait()
            shared[l][k].wait()
        swaps[(l, k, hf)].wait()
        part = dot(obuf[l, k, hf, pl.ds(own, HD)], wob[l, k, 0]) + dot(orecv[l, k, hf], wob[l, k, 1])
        send_x(l, k, hf, part)

    def add_up(l, k, hf, bias):
        crosses[(l, k, hf)].wait()
        x = xown[hf] + (xsend[l, k, hf].astype(F32) + xrecv[l, k, hf].astype(F32)) + bias
        xown[hf] = x
        return x

    def gather(l, k, hf, xn):
        rows = pl.ds(own, HD)
        xng[l, k, hf, rows] = xn
        gathers[(l, k, hf)] = remote(xng.at[l, k, hf, rows], xng.at[l, k, hf, rows], gs.at[l, k, hf], gr.at[l, k, hf], partner)

    def finish_self(l, hf):
        x = add_up(l, 0, hf, bo[l:l + 1])
        gather(l, 0, hf, norm(x, lnc[l, 0:1], lnc[l, 1:2]))

    def start_cross(l, hf):
        if hf == 0:
            weights[l][2].wait()
        gathers[(l, 0, hf)].wait()
        q = (dot(xng[l, 0, hf], wqcb[l]) + bqc[l:l + 1]).astype(BF)
        dup = jnp.where(lax.broadcasted_iota(jnp.int32, (ROWS, LANES), 0) // 2 == lax.broadcasted_iota(jnp.int32, (ROWS, LANES), 1), 1.0, 0.0).astype(BF)
        q2s[hf] = dot(dup, q).astype(BF)

    def cross_part(l, hf, sub):
        base = l * 16 + hf * 8 + sub * 4
        grp = sub + (1 - 2 * sub) * (1 - c)
        lane_id = lax.broadcasted_iota(jnp.int32, (LANES, LANES), 1)
        head_id = lax.broadcasted_iota(jnp.int32, (LANES, LANES), 0) // HD

        def body(t, _):
            n = base + t
            slot = lax.rem(n, RING)
            for m in mem_copies(n):
                m.wait()
            q = q2s[hf, pl.ds(pl.multiple_of(grp * LANES + t * 32, 32), 32), :]
            qbd = jnp.concatenate([q] * 16, axis=1) * qbm[...]
            s = dot(qbd, mkb[slot].reshape(CHUNK * LANES, ROWS)) * 0.125
            e = jnp.exp(s - jnp.max(s, axis=-1, keepdims=True))
            p = e / jnp.sum(e, axis=-1, keepdims=True)
            pm[pl.ds(pl.multiple_of(t * 32, 32), 32), :] = p.astype(BF)
            out = dot_nt(mvb[slot].reshape(CHUNK * LANES, ROWS), pm[...])
            r = racc[...]
            for i in range(CHUNK):
                r = jnp.where(lane_id == t * 32 + 2 * i + head_id, out[i * LANES:(i + 1) * LANES], r)
            racc[...] = r

            @pl.when(n + RING < 16 * L)
            def _():
                for m in mem_copies(n + RING):
                    m.start()
            return 0

        lax.fori_loop(0, 4, body, 0)
        r = jnp.where(lax.rem(lane_id, 2) == head_id, racc[...], 0.0).astype(BF)
        sel = jnp.where(lax.broadcasted_iota(jnp.int32, (HD, LANES), 1) // 2 == lax.broadcasted_iota(jnp.int32, (HD, LANES), 0), 1.0, 0.0).astype(BF)
        obuf[l, 1, hf, pl.ds(pl.multiple_of(grp * HD, HD), HD)] = dot_nt(sel, r).astype(BF)
        if sub == 0:
            send_o(l, 1, hf)

    def mlp(l, hf):
        x = add_up(l, 1, hf, boc[l:l + 1])
        xn = norm(x, lnm[l, 0:1], lnm[l, 1:2])
        if hf == 0:
            weights[l][4].wait()
            weights[l][5].wait()
            shared[l][2].wait()
            shared[l][3].wait()
            if l == 0:
                shared[0][4].wait()
        part = None
        for k in range(2):
            a = dot(xn, w1b[l, k]) + (b1 if k == 0 else b1x)[l:l + 1]
            a = (0.5 * a * (1.0 + lax.erf(a * math.sqrt(0.5)))).astype(BF)
            d = dot(a, w2b[l, k])
            part = d if part is None else part + d
        send_x(l, 2, hf, part)

    def finish_mlp(l, hf):
        x = add_up(l, 2, hf, b2[l:l + 1])
        last = l == L - 1
        params = lnf if last else lna.at[l + 1]
        gather(l, 1, hf, norm(x, params[0:1], params[1:2]))

    for l in range(L):
        self_attention(l, 0)
        self_attention(l, 1)
        if l == 0:
            for cp in caches[1]:
                cp.start()
            for cp in heads:
                cp.start()
        project(l, 0, 0)
        project(l, 0, 1)
        finish_self(l, 0)
        finish_self(l, 1)
        start_cross(l, 0)
        cross_part(l, 0, 0)
        cross_part(l, 0, 1)
        project(l, 1, 0)
        start_cross(l, 1)
        cross_part(l, 1, 0)
        mlp(l, 0)
        cross_part(l, 1, 1)
        project(l, 1, 1)
        finish_mlp(l, 0)
        mlp(l, 1)
        finish_mlp(l, 1)

    for hf in range(2):
        gathers[(L - 1, 1, hf)].wait()
        xn_out[hf * LANES:(hf + 1) * LANES, :] = xng[L - 1, 1, hf]
    for h in heads:
        h.wait()
    rows = woutb.shape[1]

    def head_body(i, carry):
        m, s = carry
        z = dot_nt(woutb[i], xn_out[...]).reshape(rows // 8, 8, ROWS)
        m2 = jnp.maximum(m, jnp.max(z, axis=0))
        s = s * jnp.exp(m - m2) + jnp.sum(jnp.exp(z - m2[None]), axis=0)
        return m2, s

    m, s = lax.fori_loop(0, HEAD_CHUNKS, head_body, (jnp.full((8, ROWS), -jnp.inf, F32), jnp.zeros((8, ROWS), F32)))
    top = jnp.max(m, axis=0, keepdims=True)
    tot = jnp.sum(s * jnp.exp(m - top), axis=0, keepdims=True)
    msb[0:8] = jnp.broadcast_to(top, (8, ROWS))
    msb[8:16] = jnp.broadcast_to(tot, (8, ROWS))
    outs = [remote(msb, msr.at[d - 1], ls.at[d - 1], lr.at[d - 1], lax.rem(me + d, 4)) for d in range(1, 4)]
    for o in outs:
        o.wait()
    big = jnp.maximum(jnp.maximum(msb[0:8], msr[0, 0:8]), jnp.maximum(msr[1, 0:8], msr[2, 0:8]))
    total = msb[8:16] * jnp.exp(msb[0:8] - big)
    for d in range(3):
        total = total + msr[d, 8:16] * jnp.exp(msr[d, 0:8] - big)
    lse_out[...] = big + jnp.log(total)


def decode(args):
    (tok, lens, kc, vc, mk, mv, lna, wqkv, bqkv, wo, bo, lnc, wqc, bqc, woc, boc, lnm, w1, b1, w2, b2, lnf, wout) = args
    L, ctx = kc.shape[:2]
    vrows = wout.shape[0] // HEAD_CHUNKS
    V = pltpu.VMEM
    dma = pltpu.SemaphoreType.DMA
    hbm = pl.BlockSpec(memory_space=pl.ANY)
    vm = pl.BlockSpec(memory_space=pltpu.VMEM)
    big = {2, 3, 4, 5, 7, 9, 12, 14, 17, 19, 22}
    return pl.pallas_call(
        decode_kernel,
        out_shape=(jax.ShapeDtypeStruct((ROWS, WIDTH), BF), jax.ShapeDtypeStruct((8, ROWS), F32),
                   jax.ShapeDtypeStruct((L, LANES, ROWS), BF), jax.ShapeDtypeStruct((L, LANES, ROWS), BF)),
        in_specs=[hbm if i in big else vm for i in range(23)],
        out_specs=(vm, vm, vm, vm),
        scratch_shapes=[
            V((RING, CHUNK, LANES, ROWS), BF), V((RING, CHUNK, LANES, ROWS), BF),
            V((ctx, LANES, ROWS), BF), V((ctx, LANES, ROWS), BF),
            V((L, 3, WIDTH, LANES), BF), V((L, 2, 2, LANES, WIDTH), BF), V((L, WIDTH, LANES), BF),
            V((L, 2, WIDTH, WIDTH), BF), V((L, 2, WIDTH, WIDTH), BF), V((HEAD_CHUNKS, vrows, WIDTH), BF), V((L, WIDTH), F32),
            V((2, HD, WIDTH), F32), V((LANES, WIDTH), BF), V((L, 2, 2, LANES, WIDTH), BF),
            V((L, 2, 2, LANES, LANES), BF), V((L, 2, 2, HD, LANES), BF),
            V((L, 3, 2, HD, WIDTH), BF), V((L, 3, 2, HD, WIDTH), BF),
            V((2, ROWS, LANES), BF), V((32, 2048), BF), V((LANES, ROWS), BF), V((LANES, LANES), F32),
            V((LANES, LANES), F32), V((LANES, LANES), F32), V((LANES, LANES), F32), V((ctx * 2, LANES), F32),
            V((16, ROWS), F32), V((3, 16, ROWS), F32),
            dma((L, 6)), dma((L, 5)), dma((L, 5)), dma((2,)), dma((RING,)), dma((RING,)), dma((HEAD_CHUNKS,)),
            dma((L, 2, 2)), dma((L, 2, 2)), dma((L, 3, 2)), dma((L, 3, 2)), dma((L, 2, 2)), dma((L, 2, 2)), dma((3,)), dma((3,)),
        ],
        compiler_params=pltpu.CompilerParams(collective_id=0, has_side_effects=True, vmem_limit_bytes=67043328),
        name='decode',
    )(*args)


def write_kernel(lens, kn, vn, kc, vc, wout, xn, lse, k_out, v_out, logp, *, blk, ctx):
    first = lax.rem(pl.program_id(0) * blk, ctx)
    for src, new, dst in ((kc, kn, k_out), (vc, vn, v_out)):
        for j in range(blk):
            hit = lens[...] == first + j
            dst[j] = jnp.where(hit, new[0], src[j])
    logp[...] = dot_nt(wout[...], xn[...]) - lse[0:1]


def write_out(lens, kn, vn, kc, vc, wout, xn, lse):
    L, ctx = kc.shape[:2]
    steps = 8
    blk = L * ctx // steps
    per = steps // L
    vocab = wout.shape[0]
    rows = -(-vocab // steps // 16) * 16
    whole = lambda a: pl.BlockSpec(a.shape, lambda i: (0,) * a.ndim)
    cache = pl.BlockSpec((blk, LANES, ROWS), lambda i: (i, 0, 0))
    fresh = pl.BlockSpec((1, LANES, ROWS), lambda i: (i // per, 0, 0))
    flat = (L * ctx, LANES, ROWS)
    k, v, logp = pl.pallas_call(
        functools.partial(write_kernel, blk=blk, ctx=ctx),
        grid=(steps,),
        out_shape=(jax.ShapeDtypeStruct(flat, BF), jax.ShapeDtypeStruct(flat, BF), jax.ShapeDtypeStruct((vocab, ROWS), F32)),
        in_specs=[whole(lens), fresh, fresh, cache, cache, pl.BlockSpec((rows, WIDTH), lambda i: (i, 0)), whole(xn), whole(lse)],
        out_specs=(cache, cache, pl.BlockSpec((rows, ROWS), lambda i: (i, 0))),
        name='write',
    )(lens, kn, vn, kc.reshape(flat), vc.reshape(flat), wout, xn, lse)
    return k.reshape(kc.shape), v.reshape(vc.shape), logp


def solution(mesh):
    cache_spec = P(None, 'dp', None, 'tp', None)
    in_specs = (P('dp', None), P('dp'), cache_spec, cache_spec, cache_spec, cache_spec,
                P(), P(None, None, None, 'tp'), P(None, None, 'tp'), P(None, 'tp', None), P(),
                P(), P(None, None, 'tp'), P(None, 'tp'), P(None, 'tp', None), P(),
                P(), P(None, None, 'tp'), P(None, 'tp'), P(None, 'tp', None), P(),
                P(), P(None, 'tp'))
    out_specs = (P('dp', 'tp'), cache_spec, cache_spec)

    def local_step(tokens, seq_lens, k_cache, v_cache, mem_k, mem_v, ln_attn, w_qkv, b_qkv, w_o, b_o, ln_cross, w_qc, b_qc, w_oc, b_oc, ln_mlp, w_fc1, b_fc1, w_fc2, b_fc2, ln_final, w_out):
        L, B, ctx, H, D = k_cache.shape
        M = mem_k.shape[2]
        lens = seq_lens.reshape(1, B)
        kc = k_cache.transpose(0, 2, 3, 4, 1).reshape(L, ctx, H * D, B)
        vc = v_cache.transpose(0, 2, 3, 4, 1).reshape(L, ctx, H * D, B)
        mk = mem_k.transpose(0, 1, 3, 4, 2).reshape(L, B, H * D, M)
        mv = mem_v.transpose(0, 1, 3, 4, 2).reshape(L, B, H * D, M)
        wout = w_out.T
        xn, lse, kn, vn = decode((tokens, lens, kc, vc, mk, mv, ln_attn, w_qkv.transpose(0, 2, 1, 3), b_qkv.transpose(1, 0, 2), w_o, b_o, ln_cross, w_qc, b_qc,
                                  w_oc, b_oc, ln_mlp, w_fc1, b_fc1, w_fc2, b_fc2, ln_final, wout))
        k, v, logp = write_out(lens, kn, vn, kc, vc, wout, xn, lse)
        back = lambda a: a.reshape(L, ctx, H, D, B).transpose(0, 4, 1, 2, 3)
        return logp.T, back(k), back(v)

    return jax.shard_map(local_step, mesh=mesh, in_specs=in_specs, out_specs=out_specs, check_vma=False)
```

```python
import functools
import math

import jax
import jax.numpy as jnp
from jax import lax
from jax.experimental import pallas as pl
from jax.experimental.pallas import tpu as pltpu
from jax.sharding import PartitionSpec as P

BF = jnp.bfloat16
F32 = jnp.float32
MESH = pl.DeviceIdType.MESH
RING = 8
CHUNK = 16
HEAD_CHUNKS = 4
LANES = 128
HD = 64
ROWS = 256
WIDTH = 512
SELF, CROSS, MLP = range(3)
A, B = range(2)


def dot(a, b):
    return jnp.dot(a, b, preferred_element_type=F32)


def dot_nt(a, b):
    return lax.dot_general(a, b, (((1,), (1,)), ((), ())), preferred_element_type=F32)


def norm(x, gain, shift):
    mean = jnp.mean(x, axis=-1, keepdims=True)
    centred = x - mean
    var = jnp.mean(centred * centred, axis=-1, keepdims=True)
    return (centred * lax.rsqrt(var + 1e-5) * gain + shift).astype(BF)


def iota(shape, dim):
    return lax.broadcasted_iota(jnp.int32, shape, dim)


def fold(x8, op):
    x8 = op(x8, pltpu.roll(x8, 4, 0))
    return op(x8, pltpu.roll(x8, 2, 0))


def decode_kernel(tok, lens, kc, vc, mk, mv, lna, wqkv, bqkv, wo, bo, lnc, wqc, bqc, woc, boc, lnm, w1, b1, w2, b2, lnf, wout,
                  xn_out, lse_out, kn_out, vn_out,
                  mkb, mvb, ckb, cvb, wqkvb, wob, wqcb, w1b, w2b, woutb, b1x,
                  xown, xng, obuf, orecv, xsend, xrecv, qTc, pcar, pm, racc, qT, kT, vT, ss, pns, zeven, zodd, msb, msr,
                  lw_sem, rws_sem, rwr_sem, c_sem, mk_sem, mv_sem, wo_sem, es, er, xs, xr, gs, gr, ls, lr):
    L = kc.shape[0]
    ctx = kc.shape[1]
    split = ctx // 8 * 4 + 4
    me = lax.axis_index('tp')
    c = lax.rem(me, 2)
    partner = me + 1 - 2 * c
    peer = lax.rem(me + 2, 4)
    own = pl.multiple_of(c * HD, HD)
    oth = pl.multiple_of((1 - c) * HD, HD)

    def seq_chunk(n):
        layer = n // 16
        within = n % 16
        half = within // 8
        sub = (within % 8) // 4
        grp = sub + (1 - 2 * sub) * (1 - c)
        seq = half * LANES + grp * HD + (within % 4) * CHUNK
        return layer, seq

    def mem_copy(n, src, dst, sem):
        layer, seq = seq_chunk(n)
        slot = lax.rem(n, RING)
        return pltpu.make_async_copy(src.at[layer, pl.ds(seq, CHUNK)], dst.at[slot], sem.at[slot])

    def key_copy(n):
        return mem_copy(n, mk, mkb, mk_sem)

    def value_copy(n):
        return mem_copy(n, mv, mvb, mv_sem)

    def refill(copy, n):
        @pl.when(n + RING < 16 * L)
        def _():
            copy(n + RING).start()

    def cache_copies(l):
        def piece(src, dst, i, start, size):
            part = pl.ds(start, size)
            return pltpu.make_async_copy(src.at[l, part], dst.at[part], c_sem.at[i])
        return [[piece(src, dst, 2 * i + p, p * split, (split, ctx - split)[p]) for p in range(2)]
                for i, (src, dst) in enumerate(((kc, ckb), (vc, cvb)))]

    def weight_copies(l):
        pairs = ((wqkv.at[l], wqkvb.at[l]), (wo.at[l], wob.at[l, 0, 0]), (wqc.at[l], wqcb.at[l]),
                 (woc.at[l], wob.at[l, 1, 0]), (w1.at[l], w1b.at[l, 0]), (w2.at[l], w2b.at[l, 0]))
        return [pltpu.make_async_copy(s, d, lw_sem.at[l, i]) for i, (s, d) in enumerate(pairs)]

    def shared_copies(l):
        pairs = [(wo.at[l], wob.at[l, 0, 1]), (woc.at[l], wob.at[l, 1, 1]), (w1.at[l], w1b.at[l, 1]), (w2.at[l], w2b.at[l, 1])]
        if l == 0:
            pairs.append((b1, b1x))
        return [pltpu.make_async_remote_copy(s, d, rws_sem.at[l, i], rwr_sem.at[l, i], device_id={'tp': partner}, device_id_type=MESH)
                for i, (s, d) in enumerate(pairs)]

    def head_copies():
        rows = woutb.shape[1]
        return [pltpu.make_async_copy(wout.at[pl.ds(i * rows, rows)], woutb.at[i], wo_sem.at[i]) for i in range(HEAD_CHUNKS)]

    weights = [weight_copies(l) for l in range(L)]
    shared = [shared_copies(l) for l in range(L)]
    caches = [cache_copies(l) for l in range(L)]
    heads = head_copies()

    weights[A][SELF].start()
    for group in caches[A]:
        for cp in group:
            cp.start()
    barrier = pltpu.get_barrier_semaphore()
    others = [lax.rem(me + d, 4) for d in range(1, 4)]
    for dev in others:
        pl.semaphore_signal(barrier, inc=1, device_id={'tp': dev}, device_id_type=MESH)

    def meet():
        with jax.named_scope('barrier'):
            pl.semaphore_wait(barrier, len(others))
        for w in weights[A][1:]:
            w.start()
        for group in shared:
            for cp in group:
                cp.start()

    def fetch_memory():
        for n in range(RING):
            key_copy(n).start()
            value_copy(n).start()
        for w in weights[B]:
            w.start()

    pm[...] = jnp.zeros_like(pm)
    for h in range(2):
        xown[h] = tok[pl.ds(pl.multiple_of(h * LANES + own, HD), HD), :].astype(F32)

    def self_scores(l, hf):
        lanes = pl.ds(hf * LANES, LANES)
        if l == 0:
            xn = norm(tok[hf * LANES:(hf + 1) * LANES, :].astype(F32), lna[l, 0:1], lna[l, 1:2])
        else:
            with jax.named_scope('gwait'):
                gathers[(l - 1, MLP, hf)].wait()
            xn = xng[l - 1, 1, hf]
        if hf == A:
            weights[l][SELF].wait()
        for i, ref in enumerate((qT, kT, vT)):
            y = (dot(xn, wqkvb[l, i]) + bqkv[i, l:l + 1]).astype(BF)
            ref[...] = y.astype(F32).T
        kn_out[l, :, lanes] = kT[...].astype(BF)
        vn_out[l, :, lanes] = vT[...].astype(BF)

        def k_body(t, _):
            blk = ckb[pl.ds(t * 4, 4), :, lanes].astype(F32) * qT[...][None]
            ss[pl.ds(pl.multiple_of(t * 8, 8), 8), :] = jnp.sum(blk.reshape(8, HD, LANES), axis=1) * 0.125
            return 0

        for p in range(2):
            if hf == A:
                with jax.named_scope('kcwait'):
                    caches[l][0][p].wait()
            lax.fori_loop((0, split // 4)[p], (split // 4, ctx // 4)[p], k_body, 0)
        snew = jnp.sum((qT[...] * kT[...]).reshape(2, HD, LANES), axis=1) * 0.125
        snew = jnp.concatenate([snew] * 4, axis=0)
        s = ss[...].reshape(ctx // 4, 8, LANES)
        pos = iota(s.shape, 0) * 4 + iota(s.shape, 1) // 2
        ln = lens[0:1, lanes][None]
        fresh = pos == ln
        s = jnp.where(fresh, snew[None], jnp.where(pos < ln, s, -1e30))
        m8 = fold(jnp.max(s, axis=0), jnp.maximum)
        p = jnp.exp(s - m8[None])
        l8 = fold(jnp.sum(p, axis=0), jnp.add)
        p = (p / l8[None]).astype(BF).astype(F32)
        pns[...] = fold(jnp.sum(jnp.where(fresh, p, 0.0), axis=0), jnp.add)
        ss[...] = jnp.where(fresh, 0.0, p).reshape(ctx * 2, LANES)

    def self_values(l, hf):
        lanes = pl.ds(hf * LANES, LANES)

        def v_body(t, acc):
            blk = cvb[pl.ds(t * 4, 4), :, lanes].astype(F32)
            pr = ss[pl.ds(pl.multiple_of(t * 8, 8), 8), :]
            acc = list(acc)
            for j in range(4):
                for h in range(2):
                    acc[h] = acc[h] + blk[j, h * HD:(h + 1) * HD] * pr[2 * j + h:2 * j + h + 1]
            return tuple(acc)

        acc = tuple(vT[h * HD:(h + 1) * HD, :] * pns[h:h + 1] for h in range(2))
        for p in range(2):
            if hf == A:
                with jax.named_scope('vcwait'):
                    caches[l][1][p].wait()
            acc = lax.fori_loop((0, split // 4)[p], (split // 4, ctx // 4)[p], v_body, acc)
        oT = jnp.concatenate(acc, axis=0).astype(BF).astype(F32)
        obuf[l, SELF, hf] = oT.T.astype(BF)
        send_o(l, SELF, hf)

    swaps, crosses, gathers = {}, {}, {}

    def remote(src, dst, ssem, rsem, dev):
        cp = pltpu.make_async_remote_copy(src, dst, ssem, rsem, device_id={'tp': dev}, device_id_type=MESH)
        cp.start()
        return cp

    def send_o(l, k, hf):
        swaps[(l, k, hf)] = remote(obuf.at[l, k, hf, pl.ds(oth, HD)], orecv.at[l, k, hf], es.at[l, k, hf], er.at[l, k, hf], partner)

    def send_x(l, k, hf, part):
        xsend[l, k, hf] = part.astype(BF)
        crosses[(l, k, hf)] = remote(xsend.at[l, k, hf], xrecv.at[l, k, hf], xs.at[l, k, hf], xr.at[l, k, hf], peer)

    def project(l, k, hf):
        if hf == 0:
            weights[l][2 * k + 1].wait()
            shared[l][k].wait()
        with jax.named_scope('owait'):
            swaps[(l, k, hf)].wait()
        part = dot(obuf[l, k, hf, pl.ds(own, HD)], wob[l, k, 0]) + dot(orecv[l, k, hf], wob[l, k, 1])
        send_x(l, k, hf, part)

    def add_up(l, k, hf, bias):
        with jax.named_scope('xwait'):
            crosses[(l, k, hf)].wait()
        x = xown[hf] + (xsend[l, k, hf].astype(F32) + xrecv[l, k, hf].astype(F32)) + bias
        xown[hf] = x
        return x

    def gather(l, k, hf, xn):
        rows = pl.ds(own, HD)
        ref = xng.at[l, k // 2, hf, rows]
        xng[l, k // 2, hf, rows] = xn
        gathers[(l, k, hf)] = remote(ref, ref, gs.at[l, k // 2, hf], gr.at[l, k // 2, hf], partner)

    def finish_self(l, hf):
        x = add_up(l, SELF, hf, bo[l:l + 1])
        gather(l, SELF, hf, norm(x, lnc[l, 0:1], lnc[l, 1:2]))

    def scores(n, shift, hf):
        with jax.named_scope('memwait'):
            key_copy(n).wait()
        slot = lax.rem(n, RING)
        qc = pltpu.roll(qTc[hf], lax.rem(2 * LANES - shift, LANES), 1)
        rows = []
        for i in range(CHUNK):
            q = jnp.broadcast_to(qc[:, i:i + 1], (LANES, LANES))
            halves = []
            for t in range(2):
                part = mkb[slot, i, :, t * LANES:(t + 1) * LANES].astype(F32) * q
                halves.append(jnp.sum(part.reshape(2, HD, LANES), axis=1))
            rows.append(jnp.concatenate(halves, axis=1))
        s = jnp.concatenate(rows, axis=0) * 0.125
        e = jnp.exp(s - jnp.max(s, axis=-1, keepdims=True))
        return (e / jnp.sum(e, axis=-1, keepdims=True)).astype(BF)

    def values(n, t, p):
        slot = lax.rem(n, RING)
        pm[pl.ds(pl.multiple_of(t * 32, 32), 32), :] = p
        lane = iota((HD, LANES), 1)
        r = [racc[h] for h in range(2)]
        for part in range(2):
            seqs = CHUNK // 2
            out = dot_nt(mvb[slot, part * seqs:(part + 1) * seqs].reshape(seqs * LANES, ROWS), pm[...])
            for i in range(seqs):
                for h in range(2):
                    first = i * LANES + h * HD
                    r[h] = jnp.where(lane == t * 32 + 2 * (part * seqs + i) + h, out[first:first + HD], r[h])
        for h in range(2):
            racc[h] = r[h]

    def base_of(l, hf, sub):
        return l * 16 + hf * 8 + sub * 4, (sub + (1 - 2 * sub) * (1 - c)) * HD

    def start_cross(l, hf):
        if hf == A:
            weights[l][2].wait()
        with jax.named_scope('gwait'):
            gathers[(l, SELF, hf)].wait()
        q = (dot(xng[l, SELF, hf], wqcb[l]) + bqc[l:l + 1]).astype(BF)
        qTc[hf] = q.astype(F32).T
        n, seq = base_of(l, hf, 0)
        pcar[...] = scores(n, seq, hf)
        refill(key_copy, n)

    def cross_part(l, hf, sub):
        base, seq = base_of(l, hf, sub)
        last = sub == 1

        def body(t, p):
            n = base + t
            value_copy(n).wait()
            if last:
                shift = seq + (t + 1) * CHUNK
            else:
                shift = jnp.where(t == 3, base_of(l, hf, 1)[1], seq + (t + 1) * CHUNK)
            after = scores(n + 1, shift, hf)
            values(n, t, p)
            refill(key_copy, n + 1)
            refill(value_copy, n)
            return after

        p = lax.fori_loop(0, 3 if last else 4, body, pcar[...])
        if last:
            value_copy(base + 3).wait()
            values(base + 3, 3, p)
            refill(value_copy, base + 3)
        else:
            pcar[...] = p
        lane = iota((LANES, LANES), 1)
        r = jnp.concatenate([racc[0], racc[1]], axis=0)
        r = jnp.where(lax.rem(lane, 2) == iota((LANES, LANES), 0) // HD, r, 0.0).astype(BF)
        sel = jnp.where(iota((HD, LANES), 1) // 2 == iota((HD, LANES), 0), 1.0, 0.0).astype(BF)
        obuf[l, CROSS, hf, pl.ds(pl.multiple_of(seq, HD), HD)] = dot_nt(sel, r).astype(BF)
        if not last:
            send_o(l, CROSS, hf)

    def mlp(l, hf):
        x = add_up(l, CROSS, hf, boc[l:l + 1])
        xn = norm(x, lnm[l, 0:1], lnm[l, 1:2])
        if hf == 0:
            weights[l][4].wait()
            weights[l][5].wait()
            shared[l][2].wait()
            shared[l][3].wait()
            if l == 0:
                shared[0][4].wait()
        part = None
        for k in range(2):
            a = dot(xn, w1b[l, k]) + (b1 if k == 0 else b1x)[l:l + 1]
            a = (0.5 * a * (1.0 + lax.erf(a * math.sqrt(0.5)))).astype(BF)
            d = dot(a, w2b[l, k])
            part = d if part is None else part + d
        send_x(l, MLP, hf, part)

    def finish_mlp(l, hf):
        x = add_up(l, MLP, hf, b2[l:l + 1])
        last = l == L - 1
        params = lnf if last else lna.at[l + 1]
        gather(l, MLP, hf, norm(x, params[0:1], params[1:2]))

    def run(step, *args):
        with jax.named_scope(step.__name__ + '_' + '_'.join(str(a) for a in args)):
            step(*args)

    run(self_scores, A, A)
    run(meet)
    run(self_values, A, A)
    fetch_memory()
    run(self_scores, A, B)
    run(project, A, SELF, A)
    run(self_values, A, B)
    for l in range(L):
        more = l + 1 < L
        run(finish_self, l, A)
        run(project, l, SELF, B)
        run(start_cross, l, A)
        run(cross_part, l, A, 0)
        run(finish_self, l, B)
        if more:
            for group in caches[l + 1]:
                for cp in group:
                    cp.start()
        else:
            for cp in heads:
                cp.start()
        run(cross_part, l, A, 1)
        run(project, l, CROSS, A)
        run(start_cross, l, B)
        run(cross_part, l, B, 0)
        run(mlp, l, A)
        run(cross_part, l, B, 1)
        run(project, l, CROSS, B)
        run(finish_mlp, l, A)
        if more:
            run(self_scores, l + 1, A)
            run(self_values, l + 1, A)
        run(mlp, l, B)
        if more:
            run(project, l + 1, SELF, A)
        run(finish_mlp, l, B)
        if more:
            run(self_scores, l + 1, B)
            run(self_values, l + 1, B)

    for hf in range(2):
        with jax.named_scope('gwait'):
            gathers[(L - 1, MLP, hf)].wait()
        xn_out[hf * LANES:(hf + 1) * LANES, :] = xng[L - 1, 1, hf]
    with jax.named_scope('headwait'):
        for h in heads:
            h.wait()

    zbufs = (zeven, zodd)
    with jax.named_scope('head'):
        m, total = jnp.full((8, ROWS), -jnp.inf, F32), jnp.zeros((8, ROWS), F32)
        for i in range(HEAD_CHUNKS + 1):
            m2, more = m, total
            if i > 0:
                z = zbufs[(i - 1) % 2][...].reshape(-1, 8, ROWS)
                more = total + jnp.sum(jnp.exp(z - m[None]), axis=0)
            if i < HEAD_CHUNKS:
                z = dot_nt(woutb[i], xn_out[...])
                zbufs[i % 2][...] = z
                m2 = jnp.maximum(m, jnp.max(z.reshape(-1, 8, ROWS), axis=0))
                if i > 0:
                    more = more * jnp.exp(m - m2)
            m, total = m2, more
        s = total
    top = jnp.max(m, axis=0, keepdims=True)
    tot = jnp.sum(s * jnp.exp(m - top), axis=0, keepdims=True)
    msb[0:8] = jnp.broadcast_to(top, (8, ROWS))
    msb[8:16] = jnp.broadcast_to(tot, (8, ROWS))
    outs = [remote(msb, msr.at[i], ls.at[i], lr.at[i], dev) for i, dev in enumerate(others)]
    with jax.named_scope('lsewait'):
        for o in outs:
            o.wait()
    big = msb[0:8]
    for i in range(len(others)):
        big = jnp.maximum(big, msr[i, 0:8])
    total = msb[8:16] * jnp.exp(msb[0:8] - big)
    for i in range(len(others)):
        total = total + msr[i, 8:16] * jnp.exp(msr[i, 0:8] - big)
    lse_out[...] = big + jnp.log(total)


def decode(args):
    (tok, lens, kc, vc, mk, mv, lna, wqkv, bqkv, wo, bo, lnc, wqc, bqc, woc, boc, lnm, w1, b1, w2, b2, lnf, wout) = args
    L, ctx = kc.shape[:2]
    vrows = wout.shape[0] // HEAD_CHUNKS
    V = pltpu.VMEM
    dma = pltpu.SemaphoreType.DMA
    hbm = pl.BlockSpec(memory_space=pl.ANY)
    vm = pl.BlockSpec(memory_space=pltpu.VMEM)
    big = {2, 3, 4, 5, 7, 9, 12, 14, 17, 19, 22}
    return pl.pallas_call(
        decode_kernel,
        out_shape=(jax.ShapeDtypeStruct((ROWS, WIDTH), BF), jax.ShapeDtypeStruct((8, ROWS), F32),
                   jax.ShapeDtypeStruct((L, LANES, ROWS), BF), jax.ShapeDtypeStruct((L, LANES, ROWS), BF)),
        in_specs=[hbm if i in big else vm for i in range(23)],
        out_specs=(vm, vm, vm, vm),
        scratch_shapes=[
            V((RING, CHUNK, LANES, ROWS), BF), V((RING, CHUNK, LANES, ROWS), BF),
            V((ctx, LANES, ROWS), BF), V((ctx, LANES, ROWS), BF),
            V((L, 3, WIDTH, LANES), BF), V((L, 2, 2, LANES, WIDTH), BF), V((L, WIDTH, LANES), BF),
            V((L, 2, WIDTH, WIDTH), BF), V((L, 2, WIDTH, WIDTH), BF), V((HEAD_CHUNKS, vrows, WIDTH), BF), V((L, WIDTH), F32),
            V((2, HD, WIDTH), F32), V((L, 2, 2, LANES, WIDTH), BF),
            V((L, 2, 2, LANES, LANES), BF), V((L, 2, 2, HD, LANES), BF),
            V((L, 3, 2, HD, WIDTH), BF), V((L, 3, 2, HD, WIDTH), BF),
            V((2, LANES, LANES), F32), V((32, ROWS), BF), V((LANES, ROWS), BF), V((2, HD, LANES), F32),
            V((LANES, LANES), F32), V((LANES, LANES), F32), V((LANES, LANES), F32), V((ctx * 2, LANES), F32), V((8, LANES), F32), V((vrows, ROWS), F32), V((vrows, ROWS), F32),
            V((16, ROWS), F32), V((3, 16, ROWS), F32),
            dma((L, 6)), dma((L, 5)), dma((L, 5)), dma((4,)), dma((RING,)), dma((RING,)), dma((HEAD_CHUNKS,)),
            dma((L, 2, 2)), dma((L, 2, 2)), dma((L, 3, 2)), dma((L, 3, 2)), dma((L, 2, 2)), dma((L, 2, 2)), dma((3,)), dma((3,)),
        ],
        compiler_params=pltpu.CompilerParams(collective_id=0, has_side_effects=True, vmem_limit_bytes=67043328),
        name='decode',
    )(*args)


def write_kernel(lens, kn, vn, kc, vc, wout, xn, lse, k_out, v_out, logp, *, blk, ctx):
    first = lax.rem(pl.program_id(0) * blk, ctx)
    for src, new, dst in ((kc, kn, k_out), (vc, vn, v_out)):
        for j in range(blk):
            hit = lens[...] == first + j
            dst[j] = jnp.where(hit, new[0], src[j])
    logp[...] = dot_nt(wout[...], xn[...]) - lse[0:1]


def write_out(lens, kn, vn, kc, vc, wout, xn, lse):
    L, ctx = kc.shape[:2]
    blk = 4
    steps = L * ctx // blk
    per = steps // L
    vocab = wout.shape[0]
    rows = -(-vocab // steps // 16) * 16
    last = -(-vocab // rows) - 1
    whole = lambda a: pl.BlockSpec(a.shape, lambda i: (0,) * a.ndim)
    cache = pl.BlockSpec((blk, LANES, ROWS), lambda i: (i, 0, 0))
    fresh = pl.BlockSpec((1, LANES, ROWS), lambda i: (i // per, 0, 0))
    flat = (L * ctx, LANES, ROWS)
    k, v, logp = pl.pallas_call(
        functools.partial(write_kernel, blk=blk, ctx=ctx),
        grid=(steps,),
        out_shape=(jax.ShapeDtypeStruct(flat, BF), jax.ShapeDtypeStruct(flat, BF), jax.ShapeDtypeStruct((vocab, ROWS), F32)),
        in_specs=[whole(lens), fresh, fresh, cache, cache, pl.BlockSpec((rows, WIDTH), lambda i: (jnp.minimum(i, last), 0)), whole(xn), whole(lse)],
        out_specs=(cache, cache, pl.BlockSpec((rows, ROWS), lambda i: (jnp.minimum(i, last), 0))),
        name='write',
    )(lens, kn, vn, kc.reshape(flat), vc.reshape(flat), wout, xn, lse)
    return k.reshape(kc.shape), v.reshape(vc.shape), logp


def solution(mesh):
    cache_spec = P(None, 'dp', None, 'tp', None)
    in_specs = (P('dp', None), P('dp'), cache_spec, cache_spec, cache_spec, cache_spec,
                P(), P(None, None, None, 'tp'), P(None, None, 'tp'), P(None, 'tp', None), P(),
                P(), P(None, None, 'tp'), P(None, 'tp'), P(None, 'tp', None), P(),
                P(), P(None, None, 'tp'), P(None, 'tp'), P(None, 'tp', None), P(),
                P(), P(None, 'tp'))
    out_specs = (P('dp', 'tp'), cache_spec, cache_spec)

    def local_step(tokens, seq_lens, k_cache, v_cache, mem_k, mem_v, ln_attn, w_qkv, b_qkv, w_o, b_o, ln_cross, w_qc, b_qc, w_oc, b_oc, ln_mlp, w_fc1, b_fc1, w_fc2, b_fc2, ln_final, w_out):
        L, B, ctx, H, D = k_cache.shape
        M = mem_k.shape[2]
        lens = seq_lens.reshape(1, B)
        kc = k_cache.transpose(0, 2, 3, 4, 1).reshape(L, ctx, H * D, B)
        vc = v_cache.transpose(0, 2, 3, 4, 1).reshape(L, ctx, H * D, B)
        mk = mem_k.transpose(0, 1, 3, 4, 2).reshape(L, B, H * D, M)
        mv = mem_v.transpose(0, 1, 3, 4, 2).reshape(L, B, H * D, M)
        wout = w_out.T
        xn, lse, kn, vn = decode((tokens, lens, kc, vc, mk, mv, ln_attn, w_qkv.transpose(0, 2, 1, 3), b_qkv.transpose(1, 0, 2), w_o, b_o, ln_cross, w_qc, b_qc,
                                  w_oc, b_oc, ln_mlp, w_fc1, b_fc1, w_fc2, b_fc2, ln_final, wout))
        k, v, logp = write_out(lens, kn, vn, kc, vc, wout, xn, lse)
        back = lambda a: a.reshape(L, ctx, H, D, B).transpose(0, 4, 1, 2, 3)
        return logp.T, back(k), back(v)

    return jax.shard_map(local_step, mesh=mesh, in_specs=in_specs, out_specs=out_specs, check_vma=False)
```

```python
import functools
import math

import jax
import jax.numpy as jnp
from jax import lax
from jax.experimental import pallas as pl
from jax.experimental.pallas import tpu as pltpu
from jax.sharding import PartitionSpec as P

BF = jnp.bfloat16
F32 = jnp.float32
MESH = pl.DeviceIdType.MESH
RING = 7
CHUNK = 16
HEAD_ROWS = 1552
HEAD_RING = 4
DECODE_VMEM = 37 << 20
WRITE_VMEM = 20 << 20
LANES = 128
HD = 64
ROWS = 256
WIDTH = 512
SELF, CROSS, MLP = range(3)
A, B = range(2)


def dot(a, b):
    return jnp.dot(a, b, preferred_element_type=F32)


def dot_nt(a, b):
    return lax.dot_general(a, b, (((1,), (1,)), ((), ())), preferred_element_type=F32)


def norm(x, gain, shift):
    mean = jnp.mean(x, axis=-1, keepdims=True)
    centred = x - mean
    var = jnp.mean(centred * centred, axis=-1, keepdims=True)
    return (centred * lax.rsqrt(var + 1e-5) * gain + shift).astype(BF)


def iota(shape, dim):
    return lax.broadcasted_iota(jnp.int32, shape, dim)


def fold(x8, op):
    x8 = op(x8, pltpu.roll(x8, 4, 0))
    return op(x8, pltpu.roll(x8, 2, 0))


def decode_kernel(tok, lens, kc, vc, mk, mv, lna, wqkv, bqkv, wo, bo, lnc, wqc, bqc, woc, boc, lnm, w1, b1, w2, b2, lnf, wout,
                  lse_out, kn_out, vn_out, cvb, zout,
                  mkb, mvb, ckb, wqkvb, wob, wqcb, w1b, w2b, woutb, b1x,
                  xown, xng, xfT, obuf, orecv, xsend, xrecv, qTc, pcar, pm, racc, qT, kT, vT, ss, pns, msb, msr,
                  lw_sem, rws_sem, rwr_sem, c_sem, mk_sem, mv_sem, wo_sem, es, er, xs, xr, gs, gr, ls, lr):
    L = kc.shape[0]
    ctx = kc.shape[1]
    split = ctx // 8 * 4 + 4
    me = lax.axis_index('tp')
    c = lax.rem(me, 2)
    partner = me + 1 - 2 * c
    peer = lax.rem(me + 2, 4)
    own = pl.multiple_of(c * HD, HD)
    oth = pl.multiple_of((1 - c) * HD, HD)

    def seq_chunk(n):
        layer = n // 16
        within = n % 16
        half = within // 8
        sub = (within % 8) // 4
        grp = sub + (1 - 2 * sub) * (1 - c)
        seq = half * LANES + grp * HD + (within % 4) * CHUNK
        return layer, seq

    def mem_copy(n, src, dst, sem):
        layer, seq = seq_chunk(n)
        slot = lax.rem(n, RING)
        return pltpu.make_async_copy(src.at[layer, pl.ds(seq, CHUNK)], dst.at[slot], sem.at[slot])

    def key_copy(n):
        return mem_copy(n, mk, mkb, mk_sem)

    def value_copy(n):
        return mem_copy(n, mv, mvb, mv_sem)

    def refill(copy, n):
        @pl.when(n + RING < 16 * L)
        def _():
            copy(n + RING).start()

    def cache_copies(l):
        def piece(src, dst, i, start, size):
            part = pl.ds(start, size)
            dst = dst.at[l, part] if dst is cvb else dst.at[part]
            return pltpu.make_async_copy(src.at[l, part], dst, c_sem.at[l, i])
        return [[piece(src, dst, 2 * i + p, p * split, (split, ctx - split)[p]) for p in range(2)]
                for i, (src, dst) in enumerate(((kc, ckb), (vc, cvb)))]

    def weight_copies(l):
        pairs = ((wqkv.at[l], wqkvb.at[l]), (wo.at[l], wob.at[l, 0, 0]), (wqc.at[l], wqcb.at[l]),
                 (woc.at[l], wob.at[l, 1, 0]), (w1.at[l], w1b.at[l, 0]), (w2.at[l], w2b.at[l, 0]))
        return [pltpu.make_async_copy(s, d, lw_sem.at[l, i]) for i, (s, d) in enumerate(pairs)]

    def shared_copies(l):
        pairs = [(wo.at[l], wob.at[l, 0, 1]), (woc.at[l], wob.at[l, 1, 1]), (w1.at[l], w1b.at[l, 1]), (w2.at[l], w2b.at[l, 1])]
        if l == 0:
            pairs.append((b1, b1x))
        return [pltpu.make_async_remote_copy(s, d, rws_sem.at[l, i], rwr_sem.at[l, i], device_id={'tp': partner}, device_id_type=MESH)
                for i, (s, d) in enumerate(pairs)]

    vocab = wout.shape[0]
    starts = list(range(0, vocab, HEAD_ROWS))
    sizes = [min(HEAD_ROWS, vocab - first) for first in starts]

    def head_copy(i):
        slot = i % HEAD_RING
        return pltpu.make_async_copy(wout.at[pl.ds(starts[i], sizes[i])], woutb.at[slot, pl.ds(0, sizes[i])], wo_sem.at[slot])

    weights = [weight_copies(l) for l in range(L)]
    shared = [shared_copies(l) for l in range(L)]
    caches = [cache_copies(l) for l in range(L)]

    weights[A][SELF].start()
    barrier = pltpu.get_barrier_semaphore()
    others = [lax.rem(me + d, 4) for d in range(1, 4)]
    for dev in others:
        pl.semaphore_signal(barrier, inc=1, device_id={'tp': dev}, device_id_type=MESH)

    def meet():
        with jax.named_scope('barrier'):
            pl.semaphore_wait(barrier, len(others))
        shared[A][SELF].start()
        for w in weights[A][1:]:
            w.start()

    def fetch_memory():
        for n in range(RING):
            key_copy(n).start()
            value_copy(n).start()

    def share(l):
        for cp in shared[l][1 - l:]:
            cp.start()

    pm[...] = jnp.zeros_like(pm)
    for h in range(2):
        xown[h] = tok[pl.ds(pl.multiple_of(h * LANES + own, HD), HD), :].astype(F32)

    def fetch_caches(l):
        for group in caches[l]:
            for cp in group:
                cp.start()

    def self_scores(l, hf):
        lanes = pl.ds(hf * LANES, LANES)
        if l == 0:
            xn = norm(tok[hf * LANES:(hf + 1) * LANES, :].astype(F32), lna[l, 0:1], lna[l, 1:2])
            if hf == A:
                fetch_caches(l)
        else:
            with jax.named_scope('gwait'):
                gathers[(l - 1, MLP, hf)].wait()
            xn = xng[l - 1, 1, hf]
        if hf == A:
            weights[l][SELF].wait()
        for i, ref in enumerate((qT, kT, vT)):
            y = (dot(xn, wqkvb[l, i]) + bqkv[i, l:l + 1]).astype(BF)
            ref[...] = y.astype(F32).T
        kn_out[l, :, lanes] = kT[...].astype(BF)
        vn_out[l, :, lanes] = vT[...].astype(BF)

        def k_body(t, _):
            blk = ckb[pl.ds(t * 4, 4), :, lanes].astype(F32) * qT[...][None]
            ss[pl.ds(pl.multiple_of(t * 8, 8), 8), :] = jnp.sum(blk.reshape(8, HD, LANES), axis=1) * 0.125
            return 0

        for p in range(2):
            if hf == A:
                with jax.named_scope('kcwait'):
                    caches[l][0][p].wait()
            lax.fori_loop((0, split // 4)[p], (split // 4, ctx // 4)[p], k_body, 0)
        snew = jnp.sum((qT[...] * kT[...]).reshape(2, HD, LANES), axis=1) * 0.125
        snew = jnp.concatenate([snew] * 4, axis=0)
        s = ss[...].reshape(ctx // 4, 8, LANES)
        pos = iota(s.shape, 0) * 4 + iota(s.shape, 1) // 2
        ln = lens[0:1, lanes][None]
        fresh = pos == ln
        s = jnp.where(fresh, snew[None], jnp.where(pos < ln, s, -1e30))
        m8 = fold(jnp.max(s, axis=0), jnp.maximum)
        p = jnp.exp(s - m8[None])
        l8 = fold(jnp.sum(p, axis=0), jnp.add)
        p = (p / l8[None]).astype(BF).astype(F32)
        pns[...] = fold(jnp.sum(jnp.where(fresh, p, 0.0), axis=0), jnp.add)
        ss[...] = jnp.where(fresh, 0.0, p).reshape(ctx * 2, LANES)

    def self_values(l, hf):
        lanes = pl.ds(hf * LANES, LANES)

        def v_body(t, acc):
            blk = cvb[l, pl.ds(t * 4, 4), :, lanes].astype(F32)
            pr = ss[pl.ds(pl.multiple_of(t * 8, 8), 8), :]
            acc = list(acc)
            for j in range(4):
                for h in range(2):
                    acc[h] = acc[h] + blk[j, h * HD:(h + 1) * HD] * pr[2 * j + h:2 * j + h + 1]
            return tuple(acc)

        acc = tuple(vT[h * HD:(h + 1) * HD, :] * pns[h:h + 1] for h in range(2))
        for p in range(2):
            if hf == A:
                with jax.named_scope('vcwait'):
                    caches[l][1][p].wait()
            acc = lax.fori_loop((0, split // 4)[p], (split // 4, ctx // 4)[p], v_body, acc)
        oT = jnp.concatenate(acc, axis=0).astype(BF).astype(F32)
        obuf[l, SELF, hf] = oT.T.astype(BF)
        send_o(l, SELF, hf)

    swaps, crosses, gathers = {}, {}, {}

    def remote(src, dst, ssem, rsem, dev):
        cp = pltpu.make_async_remote_copy(src, dst, ssem, rsem, device_id={'tp': dev}, device_id_type=MESH)
        cp.start()
        return cp

    def send_o(l, k, hf):
        swaps[(l, k, hf)] = remote(obuf.at[l, k, hf, pl.ds(oth, HD)], orecv.at[l, k, hf], es.at[l, k, hf], er.at[l, k, hf], partner)

    def send_x(l, k, hf, part):
        xsend[l, k, hf] = part.astype(BF)
        crosses[(l, k, hf)] = remote(xsend.at[l, k, hf], xrecv.at[l, k, hf], xs.at[l, k, hf], xr.at[l, k, hf], peer)

    def project(l, k, hf):
        if hf == 0:
            weights[l][2 * k + 1].wait()
            shared[l][k].wait()
        with jax.named_scope('owait'):
            swaps[(l, k, hf)].wait()
        part = dot(obuf[l, k, hf, pl.ds(own, HD)], wob[l, k, 0]) + dot(orecv[l, k, hf], wob[l, k, 1])
        send_x(l, k, hf, part)

    def add_up(l, k, hf, bias):
        with jax.named_scope('xwait'):
            crosses[(l, k, hf)].wait()
        x = xown[hf] + (xsend[l, k, hf].astype(F32) + xrecv[l, k, hf].astype(F32)) + bias
        xown[hf] = x
        return x

    def gather(l, k, hf, xn):
        rows = pl.ds(own, HD)
        ref = xng.at[l, k // 2, hf, rows]
        xng[l, k // 2, hf, rows] = xn
        gathers[(l, k, hf)] = remote(ref, ref, gs.at[l, k // 2, hf], gr.at[l, k // 2, hf], partner)

    def finish_self(l, hf):
        x = add_up(l, SELF, hf, bo[l:l + 1])
        gather(l, SELF, hf, norm(x, lnc[l, 0:1], lnc[l, 1:2]))

    def scores(n, shift, hf):
        with jax.named_scope('memwait'):
            key_copy(n).wait()
        slot = lax.rem(n, RING)
        qc = pltpu.roll(qTc[hf], lax.rem(2 * LANES - shift, LANES), 1)
        rows = []
        for i in range(CHUNK):
            q = jnp.broadcast_to(qc[:, i:i + 1], (LANES, LANES))
            halves = []
            for t in range(2):
                part = mkb[slot, i, :, t * LANES:(t + 1) * LANES].astype(F32) * q
                halves.append(jnp.sum(part.reshape(2, HD, LANES), axis=1))
            rows.append(jnp.concatenate(halves, axis=1))
        s = jnp.concatenate(rows, axis=0) * 0.125
        e = jnp.exp(s - jnp.max(s, axis=-1, keepdims=True))
        return (e / jnp.sum(e, axis=-1, keepdims=True)).astype(BF)

    def values(n, t, p):
        slot = lax.rem(n, RING)
        pm[pl.ds(pl.multiple_of(t * 32, 32), 32), :] = p
        lane = iota((HD, LANES), 1)
        r = [racc[h] for h in range(2)]
        for part in range(2):
            seqs = CHUNK // 2
            out = dot_nt(mvb[slot, part * seqs:(part + 1) * seqs].reshape(seqs * LANES, ROWS), pm[...])
            for i in range(seqs):
                for h in range(2):
                    first = i * LANES + h * HD
                    r[h] = jnp.where(lane == t * 32 + 2 * (part * seqs + i) + h, out[first:first + HD], r[h])
        for h in range(2):
            racc[h] = r[h]

    def base_of(l, hf, sub):
        return l * 16 + hf * 8 + sub * 4, (sub + (1 - 2 * sub) * (1 - c)) * HD

    def start_cross(l, hf):
        if hf == A:
            weights[l][2].wait()
        with jax.named_scope('gwait'):
            gathers[(l, SELF, hf)].wait()
        q = (dot(xng[l, SELF, hf], wqcb[l]) + bqc[l:l + 1]).astype(BF)
        qTc[hf] = q.astype(F32).T
        n, seq = base_of(l, hf, 0)
        pcar[...] = scores(n, seq, hf)
        refill(key_copy, n)

    def cross_part(l, hf, sub):
        base, seq = base_of(l, hf, sub)
        last = sub == 1

        def body(t, p):
            n = base + t
            value_copy(n).wait()
            if last:
                shift = seq + (t + 1) * CHUNK
            else:
                shift = jnp.where(t == 3, base_of(l, hf, 1)[1], seq + (t + 1) * CHUNK)
            after = scores(n + 1, shift, hf)
            values(n, t, p)
            refill(key_copy, n + 1)
            refill(value_copy, n)
            return after

        p = lax.fori_loop(0, 3 if last else 4, body, pcar[...])
        if last:
            value_copy(base + 3).wait()
            values(base + 3, 3, p)
            refill(value_copy, base + 3)
        else:
            pcar[...] = p
        lane = iota((LANES, LANES), 1)
        r = jnp.concatenate([racc[0], racc[1]], axis=0)
        r = jnp.where(lax.rem(lane, 2) == iota((LANES, LANES), 0) // HD, r, 0.0).astype(BF)
        sel = jnp.where(iota((HD, LANES), 1) // 2 == iota((HD, LANES), 0), 1.0, 0.0).astype(BF)
        obuf[l, CROSS, hf, pl.ds(pl.multiple_of(seq, HD), HD)] = dot_nt(sel, r).astype(BF)
        if not last:
            send_o(l, CROSS, hf)

    def mlp(l, hf):
        x = add_up(l, CROSS, hf, boc[l:l + 1])
        xn = norm(x, lnm[l, 0:1], lnm[l, 1:2])
        if hf == 0:
            weights[l][4].wait()
            weights[l][5].wait()
            shared[l][2].wait()
            shared[l][3].wait()
            if l == 0:
                shared[0][4].wait()
        part = None
        for k in range(2):
            a = dot(xn, w1b[l, k]) + (b1 if k == 0 else b1x)[l:l + 1]
            a = (0.5 * a * (1.0 + lax.erf(a * math.sqrt(0.5)))).astype(BF)
            d = dot(a, w2b[l, k])
            part = d if part is None else part + d
        send_x(l, MLP, hf, part)

    def finish_mlp(l, hf):
        x = add_up(l, MLP, hf, b2[l:l + 1])
        last = l == L - 1
        params = lnf if last else lna.at[l + 1]
        gather(l, MLP, hf, norm(x, params[0:1], params[1:2]))

    def run(step, *args):
        with jax.named_scope(step.__name__ + '_' + '_'.join(str(a) for a in args)):
            step(*args)

    run(self_scores, A, A)
    run(meet)
    run(self_values, A, A)
    fetch_memory()
    run(self_scores, A, B)
    run(project, A, SELF, A)
    run(self_values, A, B)
    run(project, A, SELF, B)
    for l in range(L):
        more = l + 1 < L
        run(finish_self, l, A)
        if l > 0:
            run(project, l, SELF, B)
        run(start_cross, l, A)
        if l == 0:
            share(A)
        run(cross_part, l, A, 0)
        run(finish_self, l, B)
        if l == 0:
            for w in weights[B]:
                w.start()
            fetch_caches(B)
        else:
            for i in range(HEAD_RING):
                head_copy(i).start()
        run(cross_part, l, A, 1)
        run(project, l, CROSS, A)
        run(start_cross, l, B)
        if l == 0:
            share(B)
        run(cross_part, l, B, 0)
        run(mlp, l, A)
        run(cross_part, l, B, 1)
        run(project, l, CROSS, B)
        run(finish_mlp, l, A)
        if more:
            run(self_scores, l + 1, A)
            run(self_values, l + 1, A)
        run(mlp, l, B)
        if more:
            run(project, l + 1, SELF, A)
        run(finish_mlp, l, B)
        if more:
            run(self_scores, l + 1, B)
            run(self_values, l + 1, B)

    for hf in range(2):
        with jax.named_scope('gwait'):
            gathers[(L - 1, MLP, hf)].wait()
        xfT[:, hf * LANES:(hf + 1) * LANES] = xng[L - 1, 1, hf].astype(F32).T.astype(BF)

    with jax.named_scope('head'):
        m, total = jnp.full((8, ROWS), -jnp.inf, F32), jnp.zeros((8, ROWS), F32)
        for i in range(len(starts) + 1):
            m2, more = m, total
            if i > 0:
                z = zout[starts[i - 1]:starts[i - 1] + sizes[i - 1], :].reshape(-1, 8, ROWS)
                more = total + jnp.sum(jnp.exp(z - m[None]), axis=0)
            if i < len(starts):
                head_copy(i).wait()
                z = dot(woutb[i % HEAD_RING, 0:sizes[i]], xfT[...])
                zout[starts[i]:starts[i] + sizes[i], :] = z
                if i + HEAD_RING < len(starts):
                    head_copy(i + HEAD_RING).start()
                m2 = jnp.maximum(m, jnp.max(z.reshape(-1, 8, ROWS), axis=0))
                if i > 0:
                    more = more * jnp.exp(m - m2)
            m, total = m2, more
        s = total
    top = jnp.max(m, axis=0, keepdims=True)
    tot = jnp.sum(s * jnp.exp(m - top), axis=0, keepdims=True)
    msb[0:8] = jnp.broadcast_to(top, (8, ROWS))
    msb[8:16] = jnp.broadcast_to(tot, (8, ROWS))
    outs = [remote(msb, msr.at[i], ls.at[i], lr.at[i], dev) for i, dev in enumerate(others)]
    with jax.named_scope('lsewait'):
        for o in outs:
            o.wait()
    big = msb[0:8]
    for i in range(len(others)):
        big = jnp.maximum(big, msr[i, 0:8])
    total = msb[8:16] * jnp.exp(msb[0:8] - big)
    for i in range(len(others)):
        total = total + msr[i, 8:16] * jnp.exp(msr[i, 0:8] - big)
    lse_out[...] = big + jnp.log(total)


def decode(args):
    (tok, lens, kc, vc, mk, mv, lna, wqkv, bqkv, wo, bo, lnc, wqc, bqc, woc, boc, lnm, w1, b1, w2, b2, lnf, wout) = args
    L, ctx = kc.shape[:2]
    V = pltpu.VMEM
    dma = pltpu.SemaphoreType.DMA
    hbm = pl.BlockSpec(memory_space=pltpu.HBM)
    vm = pl.BlockSpec(memory_space=V)
    streamed = [kc, vc, mk, mv, wqkv, wo, wqc, woc, w1, w2, wout]
    return pl.pallas_call(
        decode_kernel,
        out_shape=(V((8, ROWS), F32), V((L, LANES, ROWS), BF), V((L, LANES, ROWS), BF),
                   V(vc.shape, BF), V((wout.shape[0], ROWS), F32)),
        in_specs=[hbm if any(a is b for b in streamed) else vm for a in args],
        out_specs=(vm,) * 5,
        scratch_shapes=[
            V((RING, CHUNK, LANES, ROWS), BF), V((RING, CHUNK, LANES, ROWS), BF), V(kc.shape[1:], BF),
            V((L, 3, WIDTH, LANES), BF), V((L, 2, 2, LANES, WIDTH), BF), V((L, WIDTH, LANES), BF),
            V((L, 2, WIDTH, WIDTH), BF), V((L, 2, WIDTH, WIDTH), BF), V((HEAD_RING, HEAD_ROWS, WIDTH), BF), V((L, WIDTH), F32),
            V((2, HD, WIDTH), F32), V((L, 2, 2, LANES, WIDTH), BF), V((WIDTH, ROWS), BF),
            V((L, 2, 2, LANES, LANES), BF), V((L, 2, 2, HD, LANES), BF),
            V((L, 3, 2, HD, WIDTH), BF), V((L, 3, 2, HD, WIDTH), BF),
            V((2, LANES, LANES), F32), V((32, ROWS), BF), V((LANES, ROWS), BF), V((2, HD, LANES), F32),
            V((LANES, LANES), F32), V((LANES, LANES), F32), V((LANES, LANES), F32), V((ctx * 2, LANES), F32), V((8, LANES), F32),
            V((16, ROWS), F32), V((3, 16, ROWS), F32),
            dma((L, 6)), dma((L, 5)), dma((L, 5)), dma((L, 4)), dma((RING,)), dma((RING,)), dma((HEAD_RING,)),
            dma((L, 2, 2)), dma((L, 2, 2)), dma((L, 3, 2)), dma((L, 3, 2)), dma((L, 2, 2)), dma((L, 2, 2)), dma((3,)), dma((3,)),
        ],
        compiler_params=pltpu.CompilerParams(collective_id=0, has_side_effects=True, vmem_limit_bytes=DECODE_VMEM),
        name='decode',
    )(*args)


def write_kernel(lens, kn, vn, kc, vc, z, lse, k_out, v_out, logp, kb, vb, zb, k_sem, v_sem, z_sem):
    L, ctx = kc.shape[:2]
    slots, blk = vb.shape[:2]
    per = ctx // blk
    steps = L * per
    vocab = z.shape[0]
    starts = list(range(0, vocab, HEAD_ROWS))

    def key_read(i):
        part = pl.ds((i % per) * blk, blk)
        return pltpu.make_async_copy(kc.at[i // per, part], kb.at[i // per, part], k_sem.at[i])

    def key_copy(i):
        part = pl.ds((i % per) * blk, blk)
        return pltpu.make_async_copy(kb.at[i // per, part], k_out.at[i // per, part], k_sem.at[steps + i])

    def value_copy(i):
        return pltpu.make_async_copy(vb.at[i % slots], v_out.at[i // per, pl.ds((i % per) * blk, blk)], v_sem.at[i % slots])

    def logp_copy(i):
        size = min(HEAD_ROWS, vocab - starts[i])
        return pltpu.make_async_copy(zb.at[i % slots, pl.ds(0, size)], logp.at[pl.ds(starts[i], size)], z_sem.at[i % slots])

    for i in range(steps):
        key_read(i).start()
    for i in range(steps):
        slot, l, first = i % slots, i // per, (i % per) * blk
        if i >= slots:
            value_copy(i - slots).wait()
            logp_copy(i - slots).wait()

        def edit_value(j, _):
            vb[slot, j] = jnp.where(lens[...] == first + j, vn[l], vc[l, first + j])
            return 0

        def edit_key(j, _):
            kb[l, first + j] = jnp.where(lens[...] == first + j, kn[l], kb[l, first + j])
            return 0

        lax.fori_loop(0, blk, edit_value, 0)
        value_copy(i).start()
        size = min(HEAD_ROWS, vocab - starts[i])
        zb[slot, 0:size, :] = z[starts[i]:starts[i] + size, :] - lse[0:1]
        logp_copy(i).start()
        key_read(i).wait()
        lax.fori_loop(0, blk, edit_key, 0)
        key_copy(i).start()
    for i in range(steps):
        key_copy(i).wait()
    for i in range(steps - slots, steps):
        value_copy(i).wait()
        logp_copy(i).wait()


def write_out(lens, kn, vn, kc, vc, z, lse):
    L, ctx = kc.shape[:2]
    V = pltpu.VMEM
    dma = pltpu.SemaphoreType.DMA
    slots, blk = 2, ctx // 4
    vm, hbm = pl.BlockSpec(memory_space=V), pl.BlockSpec(memory_space=pltpu.HBM)
    cache = V((slots, blk) + kc.shape[2:], BF)
    like = lambda a: jax.ShapeDtypeStruct(a.shape, a.dtype)
    return pl.pallas_call(
        write_kernel,
        out_shape=(like(kc), like(vc), like(z)),
        in_specs=[vm, vm, vm, hbm, vm, vm, vm],
        out_specs=(hbm,) * 3,
        scratch_shapes=[V(kc.shape, BF), cache, V((slots, HEAD_ROWS, ROWS), F32), dma((2 * L * (ctx // blk),)), dma((slots,)), dma((slots,))],
        compiler_params=pltpu.CompilerParams(vmem_limit_bytes=WRITE_VMEM),
        name='write',
    )(lens, kn, vn, kc, vc, z, lse)


def solution(mesh):
    cache_spec = P(None, 'dp', None, 'tp', None)
    in_specs = (P('dp', None), P('dp'), cache_spec, cache_spec, cache_spec, cache_spec,
                P(), P(None, None, None, 'tp'), P(None, None, 'tp'), P(None, 'tp', None), P(),
                P(), P(None, None, 'tp'), P(None, 'tp'), P(None, 'tp', None), P(),
                P(), P(None, None, 'tp'), P(None, 'tp'), P(None, 'tp', None), P(),
                P(), P(None, 'tp'))
    out_specs = (P('dp', 'tp'), cache_spec, cache_spec)

    def local_step(tokens, seq_lens, k_cache, v_cache, mem_k, mem_v, ln_attn, w_qkv, b_qkv, w_o, b_o, ln_cross, w_qc, b_qc, w_oc, b_oc, ln_mlp, w_fc1, b_fc1, w_fc2, b_fc2, ln_final, w_out):
        L, B, ctx, H, D = k_cache.shape
        M = mem_k.shape[2]
        lens = seq_lens.reshape(1, B)
        kc = k_cache.transpose(0, 2, 3, 4, 1).reshape(L, ctx, H * D, B)
        vc = v_cache.transpose(0, 2, 3, 4, 1).reshape(L, ctx, H * D, B)
        mk = mem_k.transpose(0, 1, 3, 4, 2).reshape(L, B, H * D, M)
        mv = mem_v.transpose(0, 1, 3, 4, 2).reshape(L, B, H * D, M)
        wout = w_out.T
        lse, kn, vn, held, z = decode((tokens, lens, kc, vc, mk, mv, ln_attn, w_qkv.transpose(0, 2, 1, 3), b_qkv.transpose(1, 0, 2), w_o, b_o, ln_cross, w_qc, b_qc,
                                  w_oc, b_oc, ln_mlp, w_fc1, b_fc1, w_fc2, b_fc2, ln_final, wout))
        k, v, logp = write_out(lens, kn, vn, kc, held, z, lse)
        back = lambda a: a.reshape(L, ctx, H, D, B).transpose(0, 4, 1, 2, 3)
        return logp.T, back(k), back(v)

    return jax.shard_map(local_step, mesh=mesh, in_specs=in_specs, out_specs=out_specs, check_vma=False)
```

```python
import functools
import math

import jax
import jax.numpy as jnp
from jax import lax
from jax.experimental import pallas as pl
from jax.experimental.pallas import tpu as pltpu
from jax.sharding import PartitionSpec as P

BF = jnp.bfloat16
F32 = jnp.float32
MESH = pl.DeviceIdType.MESH
RING = 9
CHUNK = 16
HEAD_ROWS = 2048
Z_ROWS = 1552
DECODE_VMEM = 36 << 20
WRITE_VMEM = 20 << 20
LANES = 128
HD = 64
ROWS = 256
WIDTH = 512
SELF, CROSS, MLP = range(3)
A, B = range(2)


def dot(a, b):
    return jnp.dot(a, b, preferred_element_type=F32)


def dot_nt(a, b):
    return lax.dot_general(a, b, (((1,), (1,)), ((), ())), preferred_element_type=F32)


def norm(x, gain, shift):
    mean = jnp.mean(x, axis=-1, keepdims=True)
    centred = x - mean
    var = jnp.mean(centred * centred, axis=-1, keepdims=True)
    return (centred * lax.rsqrt(var + 1e-5) * gain + shift).astype(BF)


def iota(shape, dim):
    return lax.broadcasted_iota(jnp.int32, shape, dim)


def fold(x8, op):
    x8 = op(x8, pltpu.roll(x8, 4, 0))
    return op(x8, pltpu.roll(x8, 2, 0))


def decode_kernel(tok, lens, kc, vc, mk, mv, lna, wqkv, bqkv, wo, bo, lnc, wqc, bqc, woc, boc, lnm, w1, b1, w2, b2, lnf, wout,
                  lse_out, kn_out, vn_out, cvb, zout,
                  mkb, mvb, ckb, wqkvb, wob, wqcb, w1b, w2b, b1x,
                  xown, xng, xfT, obuf, orecv, xsend, xrecv, qTc, pcar, pm, racc, qT, kT, vT, ss, pns, msb, msr,
                  lw_sem, rws_sem, rwr_sem, c_sem, mk_sem, mv_sem, es, er, xs, xr, gs, gr, ls, lr):
    L = kc.shape[0]
    ctx = kc.shape[1]
    split = ctx // 8 * 4 + 4
    me = lax.axis_index('tp')
    c = lax.rem(me, 2)
    partner = me + 1 - 2 * c
    peer = lax.rem(me + 2, 4)
    own = pl.multiple_of(c * HD, HD)
    oth = pl.multiple_of((1 - c) * HD, HD)

    def seq_chunk(n):
        layer = n // 16
        within = n % 16
        half = within // 8
        sub = (within % 8) // 4
        grp = sub + (1 - 2 * sub) * (1 - c)
        seq = half * LANES + grp * HD + (within % 4) * CHUNK
        return layer, seq

    def mem_copy(n, src, dst, sem):
        layer, seq = seq_chunk(n)
        slot = lax.rem(n, RING)
        return pltpu.make_async_copy(src.at[layer, pl.ds(seq * LANES, CHUNK * LANES)], dst.at[slot], sem.at[slot])

    def key_copy(n):
        return mem_copy(n, mk, mkb, mk_sem)

    def value_copy(n):
        return mem_copy(n, mv, mvb, mv_sem)

    def refill(copy, n):
        @pl.when(n + RING < 16 * L)
        def _():
            copy(n + RING).start()

    def cache_copies(l):
        def piece(src, dst, i, start, size):
            part = pl.ds(start, size)
            dst = dst.at[l, part] if dst is cvb else dst.at[part]
            return pltpu.make_async_copy(src.at[l, part], dst, c_sem.at[l, i])
        return [[piece(src, dst, 2 * i + p, p * split, (split, ctx - split)[p]) for p in range(2)]
                for i, (src, dst) in enumerate(((kc, ckb), (vc, cvb)))]

    def weight_copies(l):
        pairs = ((wqkv.at[l], wqkvb.at[l]), (wo.at[l], wob.at[l, 0, 0]), (wqc.at[l], wqcb.at[l]),
                 (woc.at[l], wob.at[l, 1, 0]), (w1.at[l], w1b.at[l, 0]), (w2.at[l], w2b.at[l, 0]))
        return [pltpu.make_async_copy(s, d, lw_sem.at[l, i]) for i, (s, d) in enumerate(pairs)]

    def shared_copies(l):
        pairs = [(wo.at[l], wob.at[l, 0, 1]), (woc.at[l], wob.at[l, 1, 1]), (w1.at[l], w1b.at[l, 1]), (w2.at[l], w2b.at[l, 1])]
        if l == 0:
            pairs.append((b1, b1x))
        return [pltpu.make_async_remote_copy(s, d, rws_sem.at[l, i], rwr_sem.at[l, i], device_id={'tp': partner}, device_id_type=MESH)
                for i, (s, d) in enumerate(pairs)]

    vocab = wout.shape[0]
    starts = list(range(0, vocab, HEAD_ROWS))
    sizes = [min(HEAD_ROWS, vocab - first) for first in starts]

    def head_copies(i):
        rows = pl.ds(starts[i], sizes[i])
        return [pltpu.make_async_copy(wout.at[rows, pl.ds(t * ROWS, ROWS)], dst.at[i, pl.ds(0, sizes[i])], sem.at[i])
                for t, (dst, sem) in enumerate(((mkb, mk_sem), (mvb, mv_sem)))]

    weights = [weight_copies(l) for l in range(L)]
    shared = [shared_copies(l) for l in range(L)]
    caches = [cache_copies(l) for l in range(L)]

    weights[A][SELF].start()
    barrier = pltpu.get_barrier_semaphore()
    others = [lax.rem(me + d, 4) for d in range(1, 4)]
    for dev in others:
        pl.semaphore_signal(barrier, inc=1, device_id={'tp': dev}, device_id_type=MESH)

    def meet():
        with jax.named_scope('barrier'):
            pl.semaphore_wait(barrier, len(others))
        shared[A][SELF].start()
        for w in weights[A][1:]:
            w.start()

    def fetch_memory():
        for n in range(RING):
            key_copy(n).start()
            value_copy(n).start()

    def share(l):
        for cp in shared[l][1 - l:]:
            cp.start()

    pm[...] = jnp.zeros_like(pm)
    for h in range(2):
        xown[h] = tok[pl.ds(pl.multiple_of(h * LANES + own, HD), HD), :].astype(F32)

    def fetch_caches(l):
        for group in caches[l]:
            for cp in group:
                cp.start()

    def self_scores(l, hf):
        lanes = pl.ds(hf * LANES, LANES)
        if l == 0:
            xn = norm(tok[hf * LANES:(hf + 1) * LANES, :].astype(F32), lna[l, 0:1], lna[l, 1:2])
            if hf == A:
                fetch_caches(l)
        else:
            with jax.named_scope('gwait'):
                gathers[(l - 1, MLP, hf)].wait()
            xn = xng[l - 1, 1, hf]
        if hf == A:
            weights[l][SELF].wait()
        for i, ref in enumerate((qT, kT, vT)):
            y = (dot(xn, wqkvb[l, i]) + bqkv[i, l:l + 1]).astype(BF)
            ref[...] = y.astype(F32).T
        kn_out[l, :, lanes] = kT[...].astype(BF)
        vn_out[l, :, lanes] = vT[...].astype(BF)

        def k_body(t, _):
            blk = ckb[pl.ds(t * 4, 4), :, lanes].astype(F32) * qT[...][None]
            ss[pl.ds(pl.multiple_of(t * 8, 8), 8), :] = jnp.sum(blk.reshape(8, HD, LANES), axis=1) * 0.125
            return 0

        for p in range(2):
            if hf == A:
                with jax.named_scope('kcwait'):
                    caches[l][0][p].wait()
            lax.fori_loop((0, split // 4)[p], (split // 4, ctx // 4)[p], k_body, 0)
        snew = jnp.sum((qT[...] * kT[...]).reshape(2, HD, LANES), axis=1) * 0.125
        snew = jnp.concatenate([snew] * 4, axis=0)
        s = ss[...].reshape(ctx // 4, 8, LANES)
        pos = iota(s.shape, 0) * 4 + iota(s.shape, 1) // 2
        ln = lens[0:1, lanes][None]
        fresh = pos == ln
        s = jnp.where(fresh, snew[None], jnp.where(pos < ln, s, -1e30))
        m8 = fold(jnp.max(s, axis=0), jnp.maximum)
        p = jnp.exp(s - m8[None])
        l8 = fold(jnp.sum(p, axis=0), jnp.add)
        p = (p / l8[None]).astype(BF).astype(F32)
        pns[...] = fold(jnp.sum(jnp.where(fresh, p, 0.0), axis=0), jnp.add)
        ss[...] = jnp.where(fresh, 0.0, p).reshape(ctx * 2, LANES)

    def self_values(l, hf):
        lanes = pl.ds(hf * LANES, LANES)

        def v_body(t, acc):
            blk = cvb[l, pl.ds(t * 4, 4), :, lanes].astype(F32)
            pr = ss[pl.ds(pl.multiple_of(t * 8, 8), 8), :]
            acc = list(acc)
            for j in range(4):
                for h in range(2):
                    acc[h] = acc[h] + blk[j, h * HD:(h + 1) * HD] * pr[2 * j + h:2 * j + h + 1]
            return tuple(acc)

        acc = tuple(vT[h * HD:(h + 1) * HD, :] * pns[h:h + 1] for h in range(2))
        for p in range(2):
            if hf == A:
                with jax.named_scope('vcwait'):
                    caches[l][1][p].wait()
            acc = lax.fori_loop((0, split // 4)[p], (split // 4, ctx // 4)[p], v_body, acc)
        oT = jnp.concatenate(acc, axis=0).astype(BF).astype(F32)
        obuf[l, SELF, hf] = oT.T.astype(BF)
        send_o(l, SELF, hf)

    swaps, crosses, gathers = {}, {}, {}

    def remote(src, dst, ssem, rsem, dev):
        cp = pltpu.make_async_remote_copy(src, dst, ssem, rsem, device_id={'tp': dev}, device_id_type=MESH)
        cp.start()
        return cp

    def send_o(l, k, hf):
        swaps[(l, k, hf)] = remote(obuf.at[l, k, hf, pl.ds(oth, HD)], orecv.at[l, k, hf], es.at[l, k, hf], er.at[l, k, hf], partner)

    def send_x(l, k, hf, part):
        xsend[l, k, hf] = part.astype(BF)
        crosses[(l, k, hf)] = remote(xsend.at[l, k, hf], xrecv.at[l, k, hf], xs.at[l, k, hf], xr.at[l, k, hf], peer)

    def project(l, k, hf):
        if hf == 0:
            weights[l][2 * k + 1].wait()
            shared[l][k].wait()
        with jax.named_scope('owait'):
            swaps[(l, k, hf)].wait()
        part = dot(obuf[l, k, hf, pl.ds(own, HD)], wob[l, k, 0]) + dot(orecv[l, k, hf], wob[l, k, 1])
        send_x(l, k, hf, part)

    def add_up(l, k, hf, bias):
        with jax.named_scope('xwait'):
            crosses[(l, k, hf)].wait()
        x = xown[hf] + (xsend[l, k, hf].astype(F32) + xrecv[l, k, hf].astype(F32)) + bias
        xown[hf] = x
        return x

    def gather(l, k, hf, xn):
        rows = pl.ds(own, HD)
        ref = xng.at[l, k // 2, hf, rows]
        xng[l, k // 2, hf, rows] = xn
        gathers[(l, k, hf)] = remote(ref, ref, gs.at[l, k // 2, hf], gr.at[l, k // 2, hf], partner)

    def finish_self(l, hf):
        x = add_up(l, SELF, hf, bo[l:l + 1])
        gather(l, SELF, hf, norm(x, lnc[l, 0:1], lnc[l, 1:2]))

    def scores(n, shift, hf):
        with jax.named_scope('memwait'):
            key_copy(n).wait()
        slot = lax.rem(n, RING)
        qc = pltpu.roll(qTc[hf], lax.rem(2 * LANES - shift, LANES), 1)
        rows = []
        for i in range(CHUNK):
            q = jnp.broadcast_to(qc[:, i:i + 1], (LANES, LANES))
            halves = []
            for t in range(2):
                part = mkb[slot, i * LANES:(i + 1) * LANES, t * LANES:(t + 1) * LANES].astype(F32) * q
                halves.append(jnp.sum(part.reshape(2, HD, LANES), axis=1))
            rows.append(jnp.concatenate(halves, axis=1))
        s = jnp.concatenate(rows, axis=0) * 0.125
        e = jnp.exp(s - jnp.max(s, axis=-1, keepdims=True))
        return (e / jnp.sum(e, axis=-1, keepdims=True)).astype(BF)

    def values(n, t, p):
        slot = lax.rem(n, RING)
        pm[pl.ds(pl.multiple_of(t * 32, 32), 32), :] = p
        lane = iota((HD, LANES), 1)
        r = [racc[h] for h in range(2)]
        for part in range(2):
            seqs = CHUNK // 2
            out = dot_nt(mvb[slot, part * seqs * LANES:(part + 1) * seqs * LANES], pm[...])
            for i in range(seqs):
                for h in range(2):
                    first = i * LANES + h * HD
                    r[h] = jnp.where(lane == t * 32 + 2 * (part * seqs + i) + h, out[first:first + HD], r[h])
        for h in range(2):
            racc[h] = r[h]

    def base_of(l, hf, sub):
        return l * 16 + hf * 8 + sub * 4, (sub + (1 - 2 * sub) * (1 - c)) * HD

    def start_cross(l, hf):
        if hf == A:
            weights[l][2].wait()
        with jax.named_scope('gwait'):
            gathers[(l, SELF, hf)].wait()
        q = (dot(xng[l, SELF, hf], wqcb[l]) + bqc[l:l + 1]).astype(BF)
        qTc[hf] = q.astype(F32).T
        n, seq = base_of(l, hf, 0)
        pcar[...] = scores(n, seq, hf)
        refill(key_copy, n)

    def cross_part(l, hf, sub):
        base, seq = base_of(l, hf, sub)
        last = sub == 1

        def body(t, p):
            n = base + t
            value_copy(n).wait()
            if last:
                shift = seq + (t + 1) * CHUNK
            else:
                shift = jnp.where(t == 3, base_of(l, hf, 1)[1], seq + (t + 1) * CHUNK)
            after = scores(n + 1, shift, hf)
            values(n, t, p)
            refill(key_copy, n + 1)
            refill(value_copy, n)
            return after

        p = lax.fori_loop(0, 3 if last else 4, body, pcar[...])
        if last:
            value_copy(base + 3).wait()
            values(base + 3, 3, p)
            refill(value_copy, base + 3)
        else:
            pcar[...] = p
        lane = iota((LANES, LANES), 1)
        r = jnp.concatenate([racc[0], racc[1]], axis=0)
        r = jnp.where(lax.rem(lane, 2) == iota((LANES, LANES), 0) // HD, r, 0.0).astype(BF)
        sel = jnp.where(iota((HD, LANES), 1) // 2 == iota((HD, LANES), 0), 1.0, 0.0).astype(BF)
        obuf[l, CROSS, hf, pl.ds(pl.multiple_of(seq, HD), HD)] = dot_nt(sel, r).astype(BF)
        if not last:
            send_o(l, CROSS, hf)

    def mlp(l, hf):
        x = add_up(l, CROSS, hf, boc[l:l + 1])
        xn = norm(x, lnm[l, 0:1], lnm[l, 1:2])
        if hf == 0:
            weights[l][4].wait()
            weights[l][5].wait()
            shared[l][2].wait()
            shared[l][3].wait()
            if l == 0:
                shared[0][4].wait()
        part = None
        for k in range(2):
            a = dot(xn, w1b[l, k]) + (b1 if k == 0 else b1x)[l:l + 1]
            a = (0.5 * a * (1.0 + lax.erf(a * math.sqrt(0.5)))).astype(BF)
            d = dot(a, w2b[l, k])
            part = d if part is None else part + d
        send_x(l, MLP, hf, part)

    def finish_mlp(l, hf):
        x = add_up(l, MLP, hf, b2[l:l + 1])
        last = l == L - 1
        params = lnf if last else lna.at[l + 1]
        gather(l, MLP, hf, norm(x, params[0:1], params[1:2]))

    def run(step, *args):
        with jax.named_scope(step.__name__ + '_' + '_'.join(str(a) for a in args)):
            step(*args)

    run(self_scores, A, A)
    run(meet)
    run(self_values, A, A)
    fetch_memory()
    run(self_scores, A, B)
    run(project, A, SELF, A)
    run(self_values, A, B)
    run(project, A, SELF, B)
    for l in range(L):
        more = l + 1 < L
        run(finish_self, l, A)
        if l > 0:
            run(project, l, SELF, B)
        run(start_cross, l, A)
        if l == 0:
            share(A)
        run(cross_part, l, A, 0)
        run(finish_self, l, B)
        if l == 0:
            for w in weights[B]:
                w.start()
            fetch_caches(B)
        run(cross_part, l, A, 1)
        run(project, l, CROSS, A)
        run(start_cross, l, B)
        if l == 0:
            share(B)
        run(cross_part, l, B, 0)
        run(mlp, l, A)
        run(cross_part, l, B, 1)
        if not more:
            for i in range(len(starts)):
                for cp in head_copies(i):
                    cp.start()
        run(project, l, CROSS, B)
        run(finish_mlp, l, A)
        if more:
            run(self_scores, l + 1, A)
            run(self_values, l + 1, A)
        run(mlp, l, B)
        if more:
            run(project, l + 1, SELF, A)
        run(finish_mlp, l, B)
        if more:
            run(self_scores, l + 1, B)
            run(self_values, l + 1, B)

    for hf in range(2):
        with jax.named_scope('gwait'):
            gathers[(L - 1, MLP, hf)].wait()
        xfT[:, hf * LANES:(hf + 1) * LANES] = xng[L - 1, 1, hf].astype(F32).T.astype(BF)

    with jax.named_scope('headwait'):
        for i in range(len(starts)):
            for cp in head_copies(i):
                cp.wait()
    with jax.named_scope('head'):
        m, total = jnp.full((8, ROWS), -jnp.inf, F32), jnp.zeros((8, ROWS), F32)
        for i in range(len(starts) + 1):
            m2, more = m, total
            if i > 0:
                z = zout[starts[i - 1]:starts[i - 1] + sizes[i - 1], :].reshape(-1, 8, ROWS)
                more = total + jnp.sum(jnp.exp(z - m[None]), axis=0)
            if i < len(starts):
                z = dot(mkb[i, 0:sizes[i]], xfT[0:ROWS]) + dot(mvb[i, 0:sizes[i]], xfT[ROWS:WIDTH])
                zout[starts[i]:starts[i] + sizes[i], :] = z
                m2 = jnp.maximum(m, jnp.max(z.reshape(-1, 8, ROWS), axis=0))
                if i > 0:
                    more = more * jnp.exp(m - m2)
            m, total = m2, more
        s = total
    top = jnp.max(m, axis=0, keepdims=True)
    tot = jnp.sum(s * jnp.exp(m - top), axis=0, keepdims=True)
    msb[0:8] = jnp.broadcast_to(top, (8, ROWS))
    msb[8:16] = jnp.broadcast_to(tot, (8, ROWS))
    outs = [remote(msb, msr.at[i], ls.at[i], lr.at[i], dev) for i, dev in enumerate(others)]
    with jax.named_scope('lsewait'):
        for o in outs:
            o.wait()
    big = msb[0:8]
    for i in range(len(others)):
        big = jnp.maximum(big, msr[i, 0:8])
    total = msb[8:16] * jnp.exp(msb[0:8] - big)
    for i in range(len(others)):
        total = total + msr[i, 8:16] * jnp.exp(msr[i, 0:8] - big)
    lse_out[...] = big + jnp.log(total)


def decode(args):
    (tok, lens, kc, vc, mk, mv, lna, wqkv, bqkv, wo, bo, lnc, wqc, bqc, woc, boc, lnm, w1, b1, w2, b2, lnf, wout) = args
    L, ctx = kc.shape[:2]
    V = pltpu.VMEM
    dma = pltpu.SemaphoreType.DMA
    hbm = pl.BlockSpec(memory_space=pltpu.HBM)
    vm = pl.BlockSpec(memory_space=V)
    streamed = [kc, vc, mk, mv, wqkv, wo, wqc, woc, w1, w2, wout]
    return pl.pallas_call(
        decode_kernel,
        out_shape=(V((8, ROWS), F32), V((L, LANES, ROWS), BF), V((L, LANES, ROWS), BF),
                   V(vc.shape, BF), V((wout.shape[0], ROWS), F32)),
        in_specs=[hbm if any(a is b for b in streamed) else vm for a in args],
        out_specs=(vm,) * 5,
        scratch_shapes=[
            V((RING, CHUNK * LANES, ROWS), BF), V((RING, CHUNK * LANES, ROWS), BF), V(kc.shape[1:], BF),
            V((L, 3, WIDTH, LANES), BF), V((L, 2, 2, LANES, WIDTH), BF), V((L, WIDTH, LANES), BF),
            V((L, 2, WIDTH, WIDTH), BF), V((L, 2, WIDTH, WIDTH), BF), V((L, WIDTH), F32),
            V((2, HD, WIDTH), F32), V((L, 2, 2, LANES, WIDTH), BF), V((WIDTH, ROWS), BF),
            V((L, 2, 2, LANES, LANES), BF), V((L, 2, 2, HD, LANES), BF),
            V((L, 3, 2, HD, WIDTH), BF), V((L, 3, 2, HD, WIDTH), BF),
            V((2, LANES, LANES), F32), V((32, ROWS), BF), V((LANES, ROWS), BF), V((2, HD, LANES), F32),
            V((LANES, LANES), F32), V((LANES, LANES), F32), V((LANES, LANES), F32), V((ctx * 2, LANES), F32), V((8, LANES), F32),
            V((16, ROWS), F32), V((3, 16, ROWS), F32),
            dma((L, 6)), dma((L, 5)), dma((L, 5)), dma((L, 4)), dma((RING,)), dma((RING,)),
            dma((L, 2, 2)), dma((L, 2, 2)), dma((L, 3, 2)), dma((L, 3, 2)), dma((L, 2, 2)), dma((L, 2, 2)), dma((3,)), dma((3,)),
        ],
        compiler_params=pltpu.CompilerParams(collective_id=0, has_side_effects=True, vmem_limit_bytes=DECODE_VMEM),
        name='decode',
    )(*args)


def write_kernel(lens, kn, vn, kc, vc, z, lse, k_out, v_out, logp, kb, vb, zb, k_sem, v_sem, z_sem):
    L, ctx = kc.shape[:2]
    slots, blk = vb.shape[:2]
    per = ctx // blk
    steps = L * per
    vocab = z.shape[0]
    starts = list(range(0, vocab, Z_ROWS))

    def key_read(i):
        part = pl.ds((i % per) * blk, blk)
        return pltpu.make_async_copy(kc.at[i // per, part], kb.at[i // per, part], k_sem.at[i])

    def key_copy(i):
        part = pl.ds((i % per) * blk, blk)
        return pltpu.make_async_copy(kb.at[i // per, part], k_out.at[i // per, part], k_sem.at[steps + i])

    def value_copy(i):
        return pltpu.make_async_copy(vb.at[i % slots], v_out.at[i // per, pl.ds((i % per) * blk, blk)], v_sem.at[i % slots])

    def logp_copy(i):
        size = min(Z_ROWS, vocab - starts[i])
        return pltpu.make_async_copy(zb.at[i % slots, pl.ds(0, size)], logp.at[pl.ds(starts[i], size)], z_sem.at[i % slots])

    for i in range(steps):
        key_read(i).start()
    for i in range(steps):
        slot, l, first = i % slots, i // per, (i % per) * blk
        if i >= slots:
            value_copy(i - slots).wait()
            logp_copy(i - slots).wait()

        def edit_value(j, _):
            vb[slot, j] = jnp.where(lens[...] == first + j, vn[l], vc[l, first + j])
            return 0

        def edit_key(j, _):
            kb[l, first + j] = jnp.where(lens[...] == first + j, kn[l], kb[l, first + j])
            return 0

        lax.fori_loop(0, blk, edit_value, 0)
        value_copy(i).start()
        size = min(Z_ROWS, vocab - starts[i])
        zb[slot, 0:size, :] = z[starts[i]:starts[i] + size, :] - lse[0:1]
        logp_copy(i).start()
        key_read(i).wait()
        lax.fori_loop(0, blk, edit_key, 0)
        key_copy(i).start()
    for i in range(steps):
        key_copy(i).wait()
    for i in range(steps - slots, steps):
        value_copy(i).wait()
        logp_copy(i).wait()


def write_out(lens, kn, vn, kc, vc, z, lse):
    L, ctx = kc.shape[:2]
    V = pltpu.VMEM
    dma = pltpu.SemaphoreType.DMA
    slots, blk = 2, ctx // 4
    vm, hbm = pl.BlockSpec(memory_space=V), pl.BlockSpec(memory_space=pltpu.HBM)
    cache = V((slots, blk) + kc.shape[2:], BF)
    like = lambda a: jax.ShapeDtypeStruct(a.shape, a.dtype)
    return pl.pallas_call(
        write_kernel,
        out_shape=(like(kc), like(vc), like(z)),
        in_specs=[vm, vm, vm, hbm, vm, vm, vm],
        out_specs=(hbm,) * 3,
        scratch_shapes=[V(kc.shape, BF), cache, V((slots, Z_ROWS, ROWS), F32), dma((2 * L * (ctx // blk),)), dma((slots,)), dma((slots,))],
        compiler_params=pltpu.CompilerParams(vmem_limit_bytes=WRITE_VMEM),
        name='write',
    )(lens, kn, vn, kc, vc, z, lse)


def solution(mesh):
    cache_spec = P(None, 'dp', None, 'tp', None)
    in_specs = (P('dp', None), P('dp'), cache_spec, cache_spec, cache_spec, cache_spec,
                P(), P(None, None, None, 'tp'), P(None, None, 'tp'), P(None, 'tp', None), P(),
                P(), P(None, None, 'tp'), P(None, 'tp'), P(None, 'tp', None), P(),
                P(), P(None, None, 'tp'), P(None, 'tp'), P(None, 'tp', None), P(),
                P(), P(None, 'tp'))
    out_specs = (P('dp', 'tp'), cache_spec, cache_spec)

    def local_step(tokens, seq_lens, k_cache, v_cache, mem_k, mem_v, ln_attn, w_qkv, b_qkv, w_o, b_o, ln_cross, w_qc, b_qc, w_oc, b_oc, ln_mlp, w_fc1, b_fc1, w_fc2, b_fc2, ln_final, w_out):
        L, B, ctx, H, D = k_cache.shape
        M = mem_k.shape[2]
        lens = seq_lens.reshape(1, B)
        kc = k_cache.transpose(0, 2, 3, 4, 1).reshape(L, ctx, H * D, B)
        vc = v_cache.transpose(0, 2, 3, 4, 1).reshape(L, ctx, H * D, B)
        mk = mem_k.transpose(0, 1, 3, 4, 2).reshape(L, B * H * D, M)
        mv = mem_v.transpose(0, 1, 3, 4, 2).reshape(L, B * H * D, M)
        wout = w_out.T
        lse, kn, vn, held, z = decode((tokens, lens, kc, vc, mk, mv, ln_attn, w_qkv.transpose(0, 2, 1, 3), b_qkv.transpose(1, 0, 2), w_o, b_o, ln_cross, w_qc, b_qc,
                                  w_oc, b_oc, ln_mlp, w_fc1, b_fc1, w_fc2, b_fc2, ln_final, wout))
        k, v, logp = write_out(lens, kn, vn, kc, held, z, lse)
        back = lambda a: a.reshape(L, ctx, H, D, B).transpose(0, 4, 1, 2, 3)
        return logp.T, back(k), back(v)

    return jax.shard_map(local_step, mesh=mesh, in_specs=in_specs, out_specs=out_specs, check_vma=False)
```

```python
import functools
import math

import jax
import jax.numpy as jnp
from jax import lax
from jax.experimental import pallas as pl
from jax.experimental.pallas import tpu as pltpu
from jax.sharding import PartitionSpec as P

BF = jnp.bfloat16
F32 = jnp.float32
MESH = pl.DeviceIdType.MESH
RING = 8
CHUNK = 16
ON_VECTOR = 8
HEAD_ROWS = 2048
Z_ROWS = 1552
DECODE_VMEM = 30 << 20
WRITE_VMEM = 12 << 20
LANES = 128
HD = 64
ROWS = 256
WIDTH = 512
SELF, CROSS, MLP = range(3)
A, B = range(2)


def dot(a, b):
    return jnp.dot(a, b, preferred_element_type=F32)


def dot_nt(a, b):
    return lax.dot_general(a, b, (((1,), (1,)), ((), ())), preferred_element_type=F32)


def norm(x, gain, shift):
    mean = jnp.mean(x, axis=-1, keepdims=True)
    centred = x - mean
    var = jnp.mean(centred * centred, axis=-1, keepdims=True)
    return (centred * lax.rsqrt(var + 1e-5) * gain + shift).astype(BF)


def iota(shape, dim):
    return lax.broadcasted_iota(jnp.int32, shape, dim)


def fold(x8, op):
    x8 = op(x8, pltpu.roll(x8, 4, 0))
    return op(x8, pltpu.roll(x8, 2, 0))


def decode_kernel(tok, lens, kc, vc, mk, mv, lna, wqkv, bqkv, wo, bo, lnc, wqc, bqc, woc, boc, lnm, w1, b1, w2, b2, lnf, wout,
                  lse_out, kn_out, vn_out, ck0, ck1, cvb, zout,
                  mkb, mvb, wqkvb, wob, wqcb, w1b, w2b, b1x,
                  xown, xng, xfT, obuf, orecv, xsend, xrecv, qTc, q2s, qbm, pcar, pm, racc, qT, kT, vT, ss, pns, msb, msr,
                  lw_sem, rws_sem, rwr_sem, c_sem, mk_sem, mv_sem, es, er, xs, xr, gs, gr, ls, lr):
    L = kc.shape[0]
    ctx = kc.shape[1]
    split = ctx // 8 * 4 + 4
    me = lax.axis_index('tp')
    c = lax.rem(me, 2)
    partner = me + 1 - 2 * c
    peer = lax.rem(me + 2, 4)
    own = pl.multiple_of(c * HD, HD)
    oth = pl.multiple_of((1 - c) * HD, HD)

    def seq_chunk(n):
        layer = n // 16
        within = n % 16
        half = within // 8
        sub = (within % 8) // 4
        grp = sub + (1 - 2 * sub) * (1 - c)
        seq = half * LANES + grp * HD + (within % 4) * CHUNK
        return layer, seq

    def mem_copy(n, src, dst, sem):
        layer, seq = seq_chunk(n)
        slot = lax.rem(n, RING)
        return pltpu.make_async_copy(src.at[layer, pl.ds(seq * LANES, CHUNK * LANES)], dst.at[slot], sem.at[slot])

    def key_copy(n):
        return mem_copy(n, mk, mkb, mk_sem)

    def value_copy(n):
        return mem_copy(n, mv, mvb, mv_sem)

    def refill(copy, n):
        @pl.when(n + RING < 16 * L)
        def _():
            copy(n + RING).start()

    def cache_copies(l):
        def piece(src, dst, i, start, size):
            part = pl.ds(start, size)
            dst = dst.at[l, part] if dst is cvb else dst[l].at[part]
            return pltpu.make_async_copy(src.at[l, part], dst, c_sem.at[l, i])
        return [[piece(src, dst, 2 * i + p, p * split, (split, ctx - split)[p]) for p in range(2)]
                for i, (src, dst) in enumerate(((kc, (ck0, ck1)), (vc, cvb)))]

    def weight_copies(l):
        pairs = ((wqkv.at[l], wqkvb.at[l]), (wo.at[l], wob.at[l, 0, 0]), (wqc.at[l], wqcb.at[l]),
                 (woc.at[l], wob.at[l, 1, 0]), (w1.at[l], w1b.at[l, 0]), (w2.at[l], w2b.at[l, 0]))
        return [pltpu.make_async_copy(s, d, lw_sem.at[l, i]) for i, (s, d) in enumerate(pairs)]

    def shared_copies(l):
        pairs = [(wo.at[l], wob.at[l, 0, 1]), (woc.at[l], wob.at[l, 1, 1]), (w1.at[l], w1b.at[l, 1]), (w2.at[l], w2b.at[l, 1])]
        if l == 0:
            pairs.append((b1, b1x))
        return [pltpu.make_async_remote_copy(s, d, rws_sem.at[l, i], rwr_sem.at[l, i], device_id={'tp': partner}, device_id_type=MESH)
                for i, (s, d) in enumerate(pairs)]

    vocab = wout.shape[0]
    starts = list(range(0, vocab, HEAD_ROWS))
    sizes = [min(HEAD_ROWS, vocab - first) for first in starts]

    def head_copies(i):
        rows = pl.ds(starts[i], sizes[i])
        return [pltpu.make_async_copy(wout.at[rows, pl.ds(t * ROWS, ROWS)], dst.at[i, pl.ds(0, sizes[i])], sem.at[i])
                for t, (dst, sem) in enumerate(((mkb, mk_sem), (mvb, mv_sem)))]

    weights = [weight_copies(l) for l in range(L)]
    shared = [shared_copies(l) for l in range(L)]
    caches = [cache_copies(l) for l in range(L)]

    weights[A][SELF].start()
    barrier = pltpu.get_barrier_semaphore()
    others = [lax.rem(me + d, 4) for d in range(1, 4)]
    for dev in others:
        pl.semaphore_signal(barrier, inc=1, device_id={'tp': dev}, device_id_type=MESH)

    def meet():
        with jax.named_scope('barrier'):
            pl.semaphore_wait(barrier, len(others))
        shared[A][SELF].start()
        for w in weights[A][1:]:
            w.start()

    def fetch_memory():
        for n in range(RING):
            key_copy(n).start()
            value_copy(n).start()

    def share(l):
        for cp in shared[l][1 - l:]:
            cp.start()

    pm[...] = jnp.zeros_like(pm)
    qbm[...] = jnp.where(iota(qbm.shape, 1) // HD == iota(qbm.shape, 0), 1.0, 0.0).astype(BF)
    for h in range(2):
        xown[h] = tok[pl.ds(pl.multiple_of(h * LANES + own, HD), HD), :].astype(F32)

    def fetch_caches(l):
        for group in caches[l]:
            for cp in group:
                cp.start()

    def self_scores(l, hf):
        lanes = pl.ds(hf * LANES, LANES)
        if l == 0:
            xn = norm(tok[hf * LANES:(hf + 1) * LANES, :].astype(F32), lna[l, 0:1], lna[l, 1:2])
            if hf == A:
                fetch_caches(l)
        else:
            with jax.named_scope('gwait'):
                gathers[(l - 1, MLP, hf)].wait()
            xn = xng[l - 1, 1, hf]
        if hf == A:
            weights[l][SELF].wait()
        for i, ref in enumerate((qT, kT, vT)):
            y = (dot(xn, wqkvb[l, i]) + bqkv[i, l:l + 1]).astype(BF)
            ref[...] = y.astype(F32).T
        kn_out[l, :, lanes] = kT[...].astype(BF)
        vn_out[l, :, lanes] = vT[...].astype(BF)

        def k_body(t, _):
            blk = (ck0, ck1)[l][pl.ds(t * 4, 4), :, lanes].astype(F32) * qT[...][None]
            ss[pl.ds(pl.multiple_of(t * 8, 8), 8), :] = jnp.sum(blk.reshape(8, HD, LANES), axis=1) * 0.125
            return 0

        for p in range(2):
            if hf == A:
                with jax.named_scope('kcwait'):
                    caches[l][0][p].wait()
            lax.fori_loop((0, split // 4)[p], (split // 4, ctx // 4)[p], k_body, 0)
        snew = jnp.sum((qT[...] * kT[...]).reshape(2, HD, LANES), axis=1) * 0.125
        snew = jnp.concatenate([snew] * 4, axis=0)
        s = ss[...].reshape(ctx // 4, 8, LANES)
        pos = iota(s.shape, 0) * 4 + iota(s.shape, 1) // 2
        ln = lens[0:1, lanes][None]
        fresh = pos == ln
        s = jnp.where(fresh, snew[None], jnp.where(pos < ln, s, -1e30))
        m8 = fold(jnp.max(s, axis=0), jnp.maximum)
        p = jnp.exp(s - m8[None])
        l8 = fold(jnp.sum(p, axis=0), jnp.add)
        p = (p / l8[None]).astype(BF).astype(F32)
        pns[...] = fold(jnp.sum(jnp.where(fresh, p, 0.0), axis=0), jnp.add)
        ss[...] = jnp.where(fresh, 0.0, p).reshape(ctx * 2, LANES)

    def self_values(l, hf):
        lanes = pl.ds(hf * LANES, LANES)

        def v_body(t, acc):
            blk = cvb[l, pl.ds(t * 4, 4), :, lanes].astype(F32)
            pr = ss[pl.ds(pl.multiple_of(t * 8, 8), 8), :]
            acc = list(acc)
            for j in range(4):
                for h in range(2):
                    acc[h] = acc[h] + blk[j, h * HD:(h + 1) * HD] * pr[2 * j + h:2 * j + h + 1]
            return tuple(acc)

        acc = tuple(vT[h * HD:(h + 1) * HD, :] * pns[h:h + 1] for h in range(2))
        for p in range(2):
            if hf == A:
                with jax.named_scope('vcwait'):
                    caches[l][1][p].wait()
            acc = lax.fori_loop((0, split // 4)[p], (split // 4, ctx // 4)[p], v_body, acc)
        oT = jnp.concatenate(acc, axis=0).astype(BF).astype(F32)
        obuf[l, SELF, hf] = oT.T.astype(BF)
        send_o(l, SELF, hf)

    swaps, crosses, gathers = {}, {}, {}

    def remote(src, dst, ssem, rsem, dev):
        cp = pltpu.make_async_remote_copy(src, dst, ssem, rsem, device_id={'tp': dev}, device_id_type=MESH)
        cp.start()
        return cp

    def send_o(l, k, hf):
        swaps[(l, k, hf)] = remote(obuf.at[l, k, hf, pl.ds(oth, HD)], orecv.at[l, k, hf], es.at[l, k, hf], er.at[l, k, hf], partner)

    def send_x(l, k, hf, part):
        xsend[l, k, hf] = part.astype(BF)
        crosses[(l, k, hf)] = remote(xsend.at[l, k, hf], xrecv.at[l, k, hf], xs.at[l, k, hf], xr.at[l, k, hf], peer)

    def project(l, k, hf):
        if hf == 0:
            weights[l][2 * k + 1].wait()
            shared[l][k].wait()
        with jax.named_scope('owait'):
            swaps[(l, k, hf)].wait()
        part = dot(obuf[l, k, hf, pl.ds(own, HD)], wob[l, k, 0]) + dot(orecv[l, k, hf], wob[l, k, 1])
        send_x(l, k, hf, part)

    def add_up(l, k, hf, bias):
        with jax.named_scope('xwait'):
            crosses[(l, k, hf)].wait()
        x = xown[hf] + (xsend[l, k, hf].astype(F32) + xrecv[l, k, hf].astype(F32)) + bias
        xown[hf] = x
        return x

    def gather(l, k, hf, xn):
        rows = pl.ds(own, HD)
        ref = xng.at[l, k // 2, hf, rows]
        xng[l, k // 2, hf, rows] = xn
        gathers[(l, k, hf)] = remote(ref, ref, gs.at[l, k // 2, hf], gr.at[l, k // 2, hf], partner)

    def finish_self(l, hf):
        x = add_up(l, SELF, hf, bo[l:l + 1])
        gather(l, SELF, hf, norm(x, lnc[l, 0:1], lnc[l, 1:2]))

    def scores(n, shift, hf):
        with jax.named_scope('memwait'):
            key_copy(n).wait()
        slot = lax.rem(n, RING)
        qc = pltpu.roll(qTc[hf], lax.rem(2 * LANES - shift, LANES), 1)
        rows = []
        for i in range(ON_VECTOR):
            q = jnp.broadcast_to(qc[:, i:i + 1], (LANES, LANES))
            halves = []
            for t in range(2):
                part = mkb[slot, i * LANES:(i + 1) * LANES, t * LANES:(t + 1) * LANES].astype(F32) * q
                halves.append(jnp.sum(part.reshape(2, HD, LANES), axis=1))
            rows.append(jnp.concatenate(halves, axis=1))
        rest = CHUNK - ON_VECTOR
        q2 = q2s[hf, pl.ds(pl.multiple_of(2 * shift + 2 * ON_VECTOR, 16), 2 * rest), :]
        qbd = jnp.concatenate([q2] * rest, axis=1) * qbm[...]
        rows.append(dot(qbd, mkb[slot, ON_VECTOR * LANES:CHUNK * LANES]))
        s = jnp.concatenate(rows, axis=0) * 0.125
        e = jnp.exp(s - jnp.max(s, axis=-1, keepdims=True))
        return (e / jnp.sum(e, axis=-1, keepdims=True)).astype(BF)

    def values(n, t, p):
        slot = lax.rem(n, RING)
        pm[pl.ds(pl.multiple_of(t * 32, 32), 32), :] = p
        lane = iota((HD, LANES), 1)
        r = [racc[h] for h in range(2)]
        for part in range(2):
            seqs = CHUNK // 2
            out = dot_nt(mvb[slot, part * seqs * LANES:(part + 1) * seqs * LANES], pm[...])
            for i in range(seqs):
                for h in range(2):
                    first = i * LANES + h * HD
                    r[h] = jnp.where(lane == t * 32 + 2 * (part * seqs + i) + h, out[first:first + HD], r[h])
        for h in range(2):
            racc[h] = r[h]

    def base_of(l, hf, sub):
        return l * 16 + hf * 8 + sub * 4, (sub + (1 - 2 * sub) * (1 - c)) * HD

    def start_cross(l, hf):
        if hf == A:
            weights[l][2].wait()
        with jax.named_scope('gwait'):
            gathers[(l, SELF, hf)].wait()
        q = (dot(xng[l, SELF, hf], wqcb[l]) + bqc[l:l + 1]).astype(BF)
        qTc[hf] = q.astype(F32).T
        twice = jnp.where(iota((ROWS, LANES), 0) // 2 == iota((ROWS, LANES), 1), 1.0, 0.0).astype(BF)
        q2s[hf] = dot(twice, q).astype(BF)
        n, seq = base_of(l, hf, 0)
        pcar[...] = scores(n, seq, hf)
        refill(key_copy, n)

    def cross_part(l, hf, sub):
        base, seq = base_of(l, hf, sub)
        last = sub == 1

        def body(t, p):
            n = base + t
            value_copy(n).wait()
            if last:
                shift = seq + (t + 1) * CHUNK
            else:
                shift = jnp.where(t == 3, base_of(l, hf, 1)[1], seq + (t + 1) * CHUNK)
            after = scores(n + 1, shift, hf)
            values(n, t, p)
            refill(key_copy, n + 1)
            refill(value_copy, n)
            return after

        p = lax.fori_loop(0, 3 if last else 4, body, pcar[...])
        if last:
            value_copy(base + 3).wait()
            values(base + 3, 3, p)
            refill(value_copy, base + 3)
        else:
            pcar[...] = p
        lane = iota((LANES, LANES), 1)
        r = jnp.concatenate([racc[0], racc[1]], axis=0)
        r = jnp.where(lax.rem(lane, 2) == iota((LANES, LANES), 0) // HD, r, 0.0).astype(BF)
        sel = jnp.where(iota((HD, LANES), 1) // 2 == iota((HD, LANES), 0), 1.0, 0.0).astype(BF)
        obuf[l, CROSS, hf, pl.ds(pl.multiple_of(seq, HD), HD)] = dot_nt(sel, r).astype(BF)
        if not last:
            send_o(l, CROSS, hf)

    def mlp(l, hf):
        x = add_up(l, CROSS, hf, boc[l:l + 1])
        xn = norm(x, lnm[l, 0:1], lnm[l, 1:2])
        if hf == 0:
            weights[l][4].wait()
            weights[l][5].wait()
            shared[l][2].wait()
            shared[l][3].wait()
            if l == 0:
                shared[0][4].wait()
        part = None
        for k in range(2):
            a = dot(xn, w1b[l, k]) + (b1 if k == 0 else b1x)[l:l + 1]
            a = (0.5 * a * (1.0 + lax.erf(a * math.sqrt(0.5)))).astype(BF)
            d = dot(a, w2b[l, k])
            part = d if part is None else part + d
        send_x(l, MLP, hf, part)

    def finish_mlp(l, hf):
        x = add_up(l, MLP, hf, b2[l:l + 1])
        last = l == L - 1
        params = lnf if last else lna.at[l + 1]
        gather(l, MLP, hf, norm(x, params[0:1], params[1:2]))

    def run(step, *args):
        with jax.named_scope(step.__name__ + '_' + '_'.join(str(a) for a in args)):
            step(*args)

    run(self_scores, A, A)
    run(meet)
    run(self_values, A, A)
    fetch_memory()
    run(self_scores, A, B)
    run(project, A, SELF, A)
    run(self_values, A, B)
    run(project, A, SELF, B)
    for l in range(L):
        more = l + 1 < L
        run(finish_self, l, A)
        if l > 0:
            run(project, l, SELF, B)
        run(start_cross, l, A)
        if l == 0:
            share(A)
        run(cross_part, l, A, 0)
        run(finish_self, l, B)
        if l == 0:
            for w in weights[B]:
                w.start()
            fetch_caches(B)
        run(cross_part, l, A, 1)
        run(project, l, CROSS, A)
        run(start_cross, l, B)
        if l == 0:
            share(B)
        run(cross_part, l, B, 0)
        run(mlp, l, A)
        run(cross_part, l, B, 1)
        if not more:
            for i in range(len(starts)):
                for cp in head_copies(i):
                    cp.start()
        run(project, l, CROSS, B)
        run(finish_mlp, l, A)
        if more:
            run(self_scores, l + 1, A)
            run(self_values, l + 1, A)
        run(mlp, l, B)
        if more:
            run(project, l + 1, SELF, A)
        run(finish_mlp, l, B)
        if more:
            run(self_scores, l + 1, B)
            run(self_values, l + 1, B)

    for hf in range(2):
        with jax.named_scope('gwait'):
            gathers[(L - 1, MLP, hf)].wait()
        xfT[:, hf * LANES:(hf + 1) * LANES] = xng[L - 1, 1, hf].astype(F32).T.astype(BF)

    with jax.named_scope('headwait'):
        for i in range(len(starts)):
            for cp in head_copies(i):
                cp.wait()
    with jax.named_scope('head'):
        m, total = jnp.full((8, ROWS), -jnp.inf, F32), jnp.zeros((8, ROWS), F32)
        for i in range(len(starts) + 1):
            m2, more = m, total
            if i > 0:
                z = zout[starts[i - 1]:starts[i - 1] + sizes[i - 1], :].reshape(-1, 8, ROWS)
                more = total + jnp.sum(jnp.exp(z - m[None]), axis=0)
            if i < len(starts):
                z = dot(mkb[i, 0:sizes[i]], xfT[0:ROWS]) + dot(mvb[i, 0:sizes[i]], xfT[ROWS:WIDTH])
                zout[starts[i]:starts[i] + sizes[i], :] = z
                m2 = jnp.maximum(m, jnp.max(z.reshape(-1, 8, ROWS), axis=0))
                if i > 0:
                    more = more * jnp.exp(m - m2)
            m, total = m2, more
        s = total
    top = jnp.max(m, axis=0, keepdims=True)
    tot = jnp.sum(s * jnp.exp(m - top), axis=0, keepdims=True)
    msb[0:8] = jnp.broadcast_to(top, (8, ROWS))
    msb[8:16] = jnp.broadcast_to(tot, (8, ROWS))
    outs = [remote(msb, msr.at[i], ls.at[i], lr.at[i], dev) for i, dev in enumerate(others)]
    with jax.named_scope('lsewait'):
        for o in outs:
            o.wait()
    big = msb[0:8]
    for i in range(len(others)):
        big = jnp.maximum(big, msr[i, 0:8])
    total = msb[8:16] * jnp.exp(msb[0:8] - big)
    for i in range(len(others)):
        total = total + msr[i, 8:16] * jnp.exp(msr[i, 0:8] - big)
    lse_out[...] = big + jnp.log(total)


def decode(args):
    (tok, lens, kc, vc, mk, mv, lna, wqkv, bqkv, wo, bo, lnc, wqc, bqc, woc, boc, lnm, w1, b1, w2, b2, lnf, wout) = args
    L, ctx = kc.shape[:2]
    V = pltpu.VMEM
    dma = pltpu.SemaphoreType.DMA
    hbm = pl.BlockSpec(memory_space=pltpu.HBM)
    vm = pl.BlockSpec(memory_space=V)
    streamed = [kc, vc, mk, mv, wqkv, wo, wqc, woc, w1, w2, wout]
    return pl.pallas_call(
        decode_kernel,
        out_shape=(V((8, ROWS), F32), V((L, LANES, ROWS), BF), V((L, LANES, ROWS), BF),
                   V(kc.shape[1:], BF), V(kc.shape[1:], BF), V(vc.shape, BF), V((wout.shape[0], ROWS), F32)),
        in_specs=[hbm if any(a is b for b in streamed) else vm for a in args],
        out_specs=(vm,) * 7,
        scratch_shapes=[
            V((RING, CHUNK * LANES, ROWS), BF), V((RING, CHUNK * LANES, ROWS), BF),
            V((L, 3, WIDTH, LANES), BF), V((L, 2, 2, LANES, WIDTH), BF), V((L, WIDTH, LANES), BF),
            V((L, 2, WIDTH, WIDTH), BF), V((L, 2, WIDTH, WIDTH), BF), V((L, WIDTH), F32),
            V((2, HD, WIDTH), F32), V((L, 2, 2, LANES, WIDTH), BF), V((WIDTH, ROWS), BF),
            V((L, 2, 2, LANES, LANES), BF), V((L, 2, 2, HD, LANES), BF),
            V((L, 3, 2, HD, WIDTH), BF), V((L, 3, 2, HD, WIDTH), BF),
            V((2, LANES, LANES), F32), V((2, ROWS, LANES), BF), V((2 * (CHUNK - ON_VECTOR), (CHUNK - ON_VECTOR) * LANES), BF), V((32, ROWS), BF), V((LANES, ROWS), BF), V((2, HD, LANES), F32),
            V((LANES, LANES), F32), V((LANES, LANES), F32), V((LANES, LANES), F32), V((ctx * 2, LANES), F32), V((8, LANES), F32),
            V((16, ROWS), F32), V((3, 16, ROWS), F32),
            dma((L, 6)), dma((L, 5)), dma((L, 5)), dma((L, 4)), dma((RING,)), dma((RING,)),
            dma((L, 2, 2)), dma((L, 2, 2)), dma((L, 3, 2)), dma((L, 3, 2)), dma((L, 2, 2)), dma((L, 2, 2)), dma((3,)), dma((3,)),
        ],
        compiler_params=pltpu.CompilerParams(collective_id=0, has_side_effects=True, vmem_limit_bytes=DECODE_VMEM),
        name='decode',
    )(*args)


def write_kernel(lens, kn, vn, k0, k1, vc, z, lse, k_out, v_out, logp, kb, vb, zb, k_sem, v_sem, z_sem):
    L, ctx = vc.shape[:2]
    slots, blk = vb.shape[:2]
    per = ctx // blk
    steps = L * per
    vocab = z.shape[0]
    starts = list(range(0, vocab, Z_ROWS))

    def copies(i):
        slot, part = i % slots, pl.ds((i % per) * blk, blk)
        size = min(Z_ROWS, vocab - starts[i])
        return (pltpu.make_async_copy(kb.at[slot], k_out.at[i // per, part], k_sem.at[slot]),
                pltpu.make_async_copy(vb.at[slot], v_out.at[i // per, part], v_sem.at[slot]),
                pltpu.make_async_copy(zb.at[slot, pl.ds(0, size)], logp.at[pl.ds(starts[i], size)], z_sem.at[slot]))

    for i in range(steps):
        slot, l, first = i % slots, i // per, (i % per) * blk
        key_out, value_out, logp_out = copies(i)
        if i >= slots:
            for cp in copies(i - slots):
                cp.wait()

        def edit(b, src, new):
            def body(j, _):
                b[slot, j] = jnp.where(lens[...] == first + j, new[l], src[first + j])
                return 0
            lax.fori_loop(0, blk, body, 0)

        edit(kb, (k0, k1)[l], kn)
        key_out.start()
        edit(vb, vc.at[l], vn)
        value_out.start()
        size = min(Z_ROWS, vocab - starts[i])
        zb[slot, 0:size, :] = z[starts[i]:starts[i] + size, :] - lse[0:1]
        logp_out.start()
    for i in range(steps - slots, steps):
        for cp in copies(i):
            cp.wait()


def write_out(lens, kn, vn, ks, vc, z, lse):
    L, ctx = vc.shape[:2]
    V = pltpu.VMEM
    dma = pltpu.SemaphoreType.DMA
    slots, blk = 2, ctx // 4
    vm, hbm = pl.BlockSpec(memory_space=V), pl.BlockSpec(memory_space=pltpu.HBM)
    cache = V((slots, blk) + vc.shape[2:], BF)
    like = lambda a: jax.ShapeDtypeStruct(a.shape, a.dtype)
    return pl.pallas_call(
        write_kernel,
        out_shape=(like(vc), like(vc), like(z)),
        in_specs=[vm] * 8,
        out_specs=(hbm,) * 3,
        scratch_shapes=[cache, cache, V((slots, Z_ROWS, ROWS), F32), dma((slots,)), dma((slots,)), dma((slots,))],
        compiler_params=pltpu.CompilerParams(vmem_limit_bytes=WRITE_VMEM),
        name='write',
    )(lens, kn, vn, *ks, vc, z, lse)


def solution(mesh):
    cache_spec = P(None, 'dp', None, 'tp', None)
    in_specs = (P('dp', None), P('dp'), cache_spec, cache_spec, cache_spec, cache_spec,
                P(), P(None, None, None, 'tp'), P(None, None, 'tp'), P(None, 'tp', None), P(),
                P(), P(None, None, 'tp'), P(None, 'tp'), P(None, 'tp', None), P(),
                P(), P(None, None, 'tp'), P(None, 'tp'), P(None, 'tp', None), P(),
                P(), P(None, 'tp'))
    out_specs = (P('dp', 'tp'), cache_spec, cache_spec)

    def local_step(tokens, seq_lens, k_cache, v_cache, mem_k, mem_v, ln_attn, w_qkv, b_qkv, w_o, b_o, ln_cross, w_qc, b_qc, w_oc, b_oc, ln_mlp, w_fc1, b_fc1, w_fc2, b_fc2, ln_final, w_out):
        L, B, ctx, H, D = k_cache.shape
        M = mem_k.shape[2]
        lens = seq_lens.reshape(1, B)
        kc = k_cache.transpose(0, 2, 3, 4, 1).reshape(L, ctx, H * D, B)
        vc = v_cache.transpose(0, 2, 3, 4, 1).reshape(L, ctx, H * D, B)
        mk = mem_k.transpose(0, 1, 3, 4, 2).reshape(L, B * H * D, M)
        mv = mem_v.transpose(0, 1, 3, 4, 2).reshape(L, B * H * D, M)
        wout = w_out.T
        lse, kn, vn, k0, k1, held, z = decode((tokens, lens, kc, vc, mk, mv, ln_attn, w_qkv.transpose(0, 2, 1, 3), b_qkv.transpose(1, 0, 2), w_o, b_o, ln_cross, w_qc, b_qc,
                                  w_oc, b_oc, ln_mlp, w_fc1, b_fc1, w_fc2, b_fc2, ln_final, wout))
        k, v, logp = write_out(lens, kn, vn, (k0, k1), held, z, lse)
        back = lambda a: a.reshape(L, ctx, H, D, B).transpose(0, 4, 1, 2, 3)
        return logp.T, back(k), back(v)

    return jax.shard_map(local_step, mesh=mesh, in_specs=in_specs, out_specs=out_specs, check_vma=False)
```

```python
import functools
import math

import jax
import jax.numpy as jnp
from jax import lax
from jax.experimental import pallas as pl
from jax.experimental.pallas import tpu as pltpu
from jax.sharding import PartitionSpec as P

BF = jnp.bfloat16
F32 = jnp.float32
MESH = pl.DeviceIdType.MESH
RING = 8
CHUNK = 16
ON_VECTOR = 8
HEAD_ROWS = 2048
Z_ROWS = 1552
DECODE_VMEM = 30 << 20
WRITE_VMEM = 12 << 20
LANES = 128
HD = 64
ROWS = 256
WIDTH = 512
SELF, CROSS, MLP = range(3)
A, B = range(2)


def dot(a, b):
    return jnp.dot(a, b, preferred_element_type=F32)


def dot_nt(a, b):
    return lax.dot_general(a, b, (((1,), (1,)), ((), ())), preferred_element_type=F32)


def norm(x, gain, shift):
    mean = jnp.mean(x, axis=-1, keepdims=True)
    centred = x - mean
    var = jnp.mean(centred * centred, axis=-1, keepdims=True)
    return (centred * lax.rsqrt(var + 1e-5) * gain + shift).astype(BF)


def iota(shape, dim):
    return lax.broadcasted_iota(jnp.int32, shape, dim)


def fold(x8, op):
    x8 = op(x8, pltpu.roll(x8, 4, 0))
    return op(x8, pltpu.roll(x8, 2, 0))


def decode_kernel(tok, lens, kc, vc, mk, mv, lna, wqkv, bqkv, wo, bo, lnc, wqc, bqc, woc, boc, lnm, w1, b1, w2, b2, lnf, wout,
                  lse_out, kn_out, vn_out, ck0, ck1, cvb, zout,
                  mkb, mvb, wqkvb, wob, wqcb, w1b, w2b, b1x,
                  xown, xng, xfT, obuf, orecv, xsend, xrecv, qTc, q2s, qbm, pcar, pm, racc, qT, kT, vT, ss, pns, msb, msr,
                  lw_sem, rws_sem, rwr_sem, c_sem, mk_sem, mv_sem, es, er, xs, xr, gs, gr, ls, lr):
    L = kc.shape[0]
    ctx = kc.shape[1]
    split = ctx // 8 * 4 + 4
    me = lax.axis_index('tp')
    c = lax.rem(me, 2)
    partner = me + 1 - 2 * c
    peer = lax.rem(me + 2, 4)
    own = pl.multiple_of(c * HD, HD)
    oth = pl.multiple_of((1 - c) * HD, HD)

    def seq_chunk(n):
        layer = n // 16
        within = n % 16
        half = within // 8
        sub = (within % 8) // 4
        grp = sub + (1 - 2 * sub) * (1 - c)
        seq = half * LANES + grp * HD + (within % 4) * CHUNK
        return layer, seq

    def mem_copy(n, src, dst, sem):
        layer, seq = seq_chunk(n)
        slot = lax.rem(n, RING)
        return pltpu.make_async_copy(src.at[layer, pl.ds(seq * LANES, CHUNK * LANES)], dst.at[slot], sem.at[slot])

    def key_copy(n):
        return mem_copy(n, mk, mkb, mk_sem)

    def value_copy(n):
        return mem_copy(n, mv, mvb, mv_sem)

    def refill(copy, n):
        @pl.when(n + RING < 16 * L)
        def _():
            copy(n + RING).start()

    def cache_copies(l):
        def piece(src, dst, i, start, size):
            part = pl.ds(start, size)
            dst = dst.at[l, part] if dst is cvb else dst[l].at[part]
            return pltpu.make_async_copy(src.at[l, part], dst, c_sem.at[l, i])
        return [[piece(src, dst, 2 * i + p, p * split, (split, ctx - split)[p]) for p in range(2)]
                for i, (src, dst) in enumerate(((kc, (ck0, ck1)), (vc, cvb)))]

    def weight_copies(l):
        pairs = ((wqkv.at[l], wqkvb.at[l]), (wo.at[l], wob.at[l, 0, 0]), (wqc.at[l], wqcb.at[l]),
                 (woc.at[l], wob.at[l, 1, 0]), (w1.at[l], w1b.at[l, 0]), (w2.at[l], w2b.at[l, 0]))
        return [pltpu.make_async_copy(s, d, lw_sem.at[l, i]) for i, (s, d) in enumerate(pairs)]

    def shared_copies(l):
        pairs = [(wo.at[l], wob.at[l, 0, 1]), (woc.at[l], wob.at[l, 1, 1]), (w1.at[l], w1b.at[l, 1]), (w2.at[l], w2b.at[l, 1])]
        if l == 0:
            pairs.append((b1, b1x))
        return [pltpu.make_async_remote_copy(s, d, rws_sem.at[l, i], rwr_sem.at[l, i], device_id={'tp': partner}, device_id_type=MESH)
                for i, (s, d) in enumerate(pairs)]

    vocab = wout.shape[0]
    starts = list(range(0, vocab, HEAD_ROWS))
    sizes = [min(HEAD_ROWS, vocab - first) for first in starts]

    def head_copies(i):
        rows = pl.ds(starts[i], sizes[i])
        return [pltpu.make_async_copy(wout.at[rows, pl.ds(t * ROWS, ROWS)], dst.at[i, pl.ds(0, sizes[i])], sem.at[i])
                for t, (dst, sem) in enumerate(((mkb, mk_sem), (mvb, mv_sem)))]

    weights = [weight_copies(l) for l in range(L)]
    shared = [shared_copies(l) for l in range(L)]
    caches = [cache_copies(l) for l in range(L)]

    weights[A][SELF].start()
    caches[A][0][0].start()
    barrier = pltpu.get_barrier_semaphore()
    others = [lax.rem(me + d, 4) for d in range(1, 4)]
    for dev in others:
        pl.semaphore_signal(barrier, inc=1, device_id={'tp': dev}, device_id_type=MESH)

    def meet():
        with jax.named_scope('barrier'):
            pl.semaphore_wait(barrier, len(others))
        shared[A][SELF].start()
        for w in weights[A][1:]:
            w.start()

    def fetch_memory():
        for n in range(RING):
            key_copy(n).start()
            value_copy(n).start()

    def share(l):
        for cp in shared[l][1 - l:]:
            cp.start()

    def prepare():
        pm[...] = jnp.zeros_like(pm)
        qbm[...] = jnp.where(iota(qbm.shape, 1) // HD == iota(qbm.shape, 0), 1.0, 0.0).astype(BF)
        for h in range(2):
            xown[h] = tok[pl.ds(pl.multiple_of(h * LANES + own, HD), HD), :].astype(F32)

    def fetch_caches(l):
        for cp in (caches[l][0] + caches[l][1])[1 - l:]:
            cp.start()

    def self_scores(l, hf):
        lanes = pl.ds(hf * LANES, LANES)
        if l == 0:
            xn = norm(tok[hf * LANES:(hf + 1) * LANES, :].astype(F32), lna[l, 0:1], lna[l, 1:2])
            if hf == A:
                fetch_caches(l)
        else:
            with jax.named_scope('gwait'):
                gathers[(l - 1, MLP, hf)].wait()
            xn = xng[l - 1, 1, hf]
        if hf == A:
            weights[l][SELF].wait()
        for i, ref in enumerate((qT, kT, vT)):
            y = (dot(xn, wqkvb[l, i]) + bqkv[i, l:l + 1]).astype(BF)
            ref[...] = y.astype(F32).T
        kn_out[l, :, lanes] = kT[...].astype(BF)
        vn_out[l, :, lanes] = vT[...].astype(BF)

        def k_body(t, _):
            blk = (ck0, ck1)[l][pl.ds(t * 4, 4), :, lanes].astype(F32) * qT[...][None]
            ss[pl.ds(pl.multiple_of(t * 8, 8), 8), :] = jnp.sum(blk.reshape(8, HD, LANES), axis=1) * 0.125
            return 0

        for p in range(2):
            if hf == A:
                with jax.named_scope('kcwait'):
                    caches[l][0][p].wait()
            lax.fori_loop((0, split // 4)[p], (split // 4, ctx // 4)[p], k_body, 0)
        snew = jnp.sum((qT[...] * kT[...]).reshape(2, HD, LANES), axis=1) * 0.125
        snew = jnp.concatenate([snew] * 4, axis=0)
        s = ss[...].reshape(ctx // 4, 8, LANES)
        pos = iota(s.shape, 0) * 4 + iota(s.shape, 1) // 2
        ln = lens[0:1, lanes][None]
        fresh = pos == ln
        s = jnp.where(fresh, snew[None], jnp.where(pos < ln, s, -1e30))
        m8 = fold(jnp.max(s, axis=0), jnp.maximum)
        p = jnp.exp(s - m8[None])
        l8 = fold(jnp.sum(p, axis=0), jnp.add)
        p = (p / l8[None]).astype(BF).astype(F32)
        pns[...] = fold(jnp.sum(jnp.where(fresh, p, 0.0), axis=0), jnp.add)
        ss[...] = jnp.where(fresh, 0.0, p).reshape(ctx * 2, LANES)

    def self_values(l, hf):
        lanes = pl.ds(hf * LANES, LANES)

        def v_body(t, acc):
            blk = cvb[l, pl.ds(t * 4, 4), :, lanes].astype(F32)
            pr = ss[pl.ds(pl.multiple_of(t * 8, 8), 8), :]
            acc = list(acc)
            for j in range(4):
                for h in range(2):
                    acc[h] = acc[h] + blk[j, h * HD:(h + 1) * HD] * pr[2 * j + h:2 * j + h + 1]
            return tuple(acc)

        acc = tuple(vT[h * HD:(h + 1) * HD, :] * pns[h:h + 1] for h in range(2))
        for p in range(2):
            if hf == A:
                with jax.named_scope('vcwait'):
                    caches[l][1][p].wait()
            acc = lax.fori_loop((0, split // 4)[p], (split // 4, ctx // 4)[p], v_body, acc)
        oT = jnp.concatenate(acc, axis=0).astype(BF).astype(F32)
        obuf[l, SELF, hf] = oT.T.astype(BF)
        send_o(l, SELF, hf)

    swaps, crosses, gathers = {}, {}, {}

    def remote(src, dst, ssem, rsem, dev):
        cp = pltpu.make_async_remote_copy(src, dst, ssem, rsem, device_id={'tp': dev}, device_id_type=MESH)
        cp.start()
        return cp

    def send_o(l, k, hf):
        swaps[(l, k, hf)] = remote(obuf.at[l, k, hf, pl.ds(oth, HD)], orecv.at[l, k, hf], es.at[l, k, hf], er.at[l, k, hf], partner)

    def send_x(l, k, hf, part):
        xsend[l, k, hf] = part.astype(BF)
        crosses[(l, k, hf)] = remote(xsend.at[l, k, hf], xrecv.at[l, k, hf], xs.at[l, k, hf], xr.at[l, k, hf], peer)

    def project(l, k, hf):
        if hf == 0:
            weights[l][2 * k + 1].wait()
            shared[l][k].wait()
        with jax.named_scope('owait'):
            swaps[(l, k, hf)].wait()
        part = dot(obuf[l, k, hf, pl.ds(own, HD)], wob[l, k, 0]) + dot(orecv[l, k, hf], wob[l, k, 1])
        send_x(l, k, hf, part)

    def add_up(l, k, hf, bias):
        with jax.named_scope('xwait'):
            crosses[(l, k, hf)].wait()
        x = xown[hf] + (xsend[l, k, hf].astype(F32) + xrecv[l, k, hf].astype(F32)) + bias
        xown[hf] = x
        return x

    def gather(l, k, hf, xn):
        rows = pl.ds(own, HD)
        ref = xng.at[l, k // 2, hf, rows]
        xng[l, k // 2, hf, rows] = xn
        gathers[(l, k, hf)] = remote(ref, ref, gs.at[l, k // 2, hf], gr.at[l, k // 2, hf], partner)

    def finish_self(l, hf):
        x = add_up(l, SELF, hf, bo[l:l + 1])
        gather(l, SELF, hf, norm(x, lnc[l, 0:1], lnc[l, 1:2]))

    def scores(n, shift, hf):
        with jax.named_scope('memwait'):
            key_copy(n).wait()
        slot = lax.rem(n, RING)
        qc = pltpu.roll(qTc[hf], lax.rem(2 * LANES - shift, LANES), 1)
        rows = []
        for i in range(ON_VECTOR):
            q = jnp.broadcast_to(qc[:, i:i + 1], (LANES, LANES))
            halves = []
            for t in range(2):
                part = mkb[slot, i * LANES:(i + 1) * LANES, t * LANES:(t + 1) * LANES].astype(F32) * q
                halves.append(jnp.sum(part.reshape(2, HD, LANES), axis=1))
            rows.append(jnp.concatenate(halves, axis=1))
        rest = CHUNK - ON_VECTOR
        q2 = q2s[hf, pl.ds(pl.multiple_of(2 * shift + 2 * ON_VECTOR, 16), 2 * rest), :]
        qbd = jnp.concatenate([q2] * rest, axis=1) * qbm[...]
        rows.append(dot(qbd, mkb[slot, ON_VECTOR * LANES:CHUNK * LANES]))
        s = jnp.concatenate(rows, axis=0) * 0.125
        e = jnp.exp(s - jnp.max(s, axis=-1, keepdims=True))
        return (e / jnp.sum(e, axis=-1, keepdims=True)).astype(BF)

    def values(n, t, p):
        slot = lax.rem(n, RING)
        pm[pl.ds(pl.multiple_of(t * 32, 32), 32), :] = p
        lane = iota((HD, LANES), 1)
        r = [racc[h] for h in range(2)]
        for part in range(2):
            seqs = CHUNK // 2
            out = dot_nt(mvb[slot, part * seqs * LANES:(part + 1) * seqs * LANES], pm[...])
            for i in range(seqs):
                for h in range(2):
                    first = i * LANES + h * HD
                    r[h] = jnp.where(lane == t * 32 + 2 * (part * seqs + i) + h, out[first:first + HD], r[h])
        for h in range(2):
            racc[h] = r[h]

    def base_of(l, hf, sub):
        return l * 16 + hf * 8 + sub * 4, (sub + (1 - 2 * sub) * (1 - c)) * HD

    def start_cross(l, hf):
        if hf == A:
            weights[l][2].wait()
        with jax.named_scope('gwait'):
            gathers[(l, SELF, hf)].wait()
        q = (dot(xng[l, SELF, hf], wqcb[l]) + bqc[l:l + 1]).astype(BF)
        qTc[hf] = q.astype(F32).T
        twice = jnp.where(iota((ROWS, LANES), 0) // 2 == iota((ROWS, LANES), 1), 1.0, 0.0).astype(BF)
        q2s[hf] = dot(twice, q).astype(BF)
        n, seq = base_of(l, hf, 0)
        pcar[...] = scores(n, seq, hf)
        refill(key_copy, n)

    def cross_part(l, hf, sub):
        base, seq = base_of(l, hf, sub)
        last = sub == 1

        def body(t, p):
            n = base + t
            value_copy(n).wait()
            if last:
                shift = seq + (t + 1) * CHUNK
            else:
                shift = jnp.where(t == 3, base_of(l, hf, 1)[1], seq + (t + 1) * CHUNK)
            after = scores(n + 1, shift, hf)
            values(n, t, p)
            refill(key_copy, n + 1)
            refill(value_copy, n)
            return after

        p = lax.fori_loop(0, 3 if last else 4, body, pcar[...])
        if last:
            value_copy(base + 3).wait()
            values(base + 3, 3, p)
            refill(value_copy, base + 3)
        else:
            pcar[...] = p
        lane = iota((LANES, LANES), 1)
        r = jnp.concatenate([racc[0], racc[1]], axis=0)
        r = jnp.where(lax.rem(lane, 2) == iota((LANES, LANES), 0) // HD, r, 0.0).astype(BF)
        sel = jnp.where(iota((HD, LANES), 1) // 2 == iota((HD, LANES), 0), 1.0, 0.0).astype(BF)
        obuf[l, CROSS, hf, pl.ds(pl.multiple_of(seq, HD), HD)] = dot_nt(sel, r).astype(BF)
        if not last:
            send_o(l, CROSS, hf)

    def mlp(l, hf):
        x = add_up(l, CROSS, hf, boc[l:l + 1])
        xn = norm(x, lnm[l, 0:1], lnm[l, 1:2])
        if hf == 0:
            weights[l][4].wait()
            weights[l][5].wait()
            shared[l][2].wait()
            shared[l][3].wait()
            if l == 0:
                shared[0][4].wait()
        part = None
        for k in range(2):
            a = dot(xn, w1b[l, k]) + (b1 if k == 0 else b1x)[l:l + 1]
            a = (0.5 * a * (1.0 + lax.erf(a * math.sqrt(0.5)))).astype(BF)
            d = dot(a, w2b[l, k])
            part = d if part is None else part + d
        send_x(l, MLP, hf, part)

    def finish_mlp(l, hf):
        x = add_up(l, MLP, hf, b2[l:l + 1])
        last = l == L - 1
        params = lnf if last else lna.at[l + 1]
        gather(l, MLP, hf, norm(x, params[0:1], params[1:2]))

    def run(step, *args):
        with jax.named_scope(step.__name__ + '_' + '_'.join(str(a) for a in args)):
            step(*args)

    run(self_scores, A, A)
    run(meet)
    run(self_values, A, A)
    fetch_memory()
    run(self_scores, A, B)
    run(project, A, SELF, A)
    run(self_values, A, B)
    run(prepare)
    run(project, A, SELF, B)
    for l in range(L):
        more = l + 1 < L
        run(finish_self, l, A)
        if l > 0:
            run(project, l, SELF, B)
        run(start_cross, l, A)
        if l == 0:
            share(A)
        run(cross_part, l, A, 0)
        run(finish_self, l, B)
        if l == 0:
            for w in weights[B]:
                w.start()
            fetch_caches(B)
        run(cross_part, l, A, 1)
        run(project, l, CROSS, A)
        run(start_cross, l, B)
        if l == 0:
            share(B)
        run(cross_part, l, B, 0)
        run(mlp, l, A)
        run(cross_part, l, B, 1)
        if not more:
            for i in range(len(starts)):
                for cp in head_copies(i):
                    cp.start()
        run(project, l, CROSS, B)
        run(finish_mlp, l, A)
        if more:
            run(self_scores, l + 1, A)
        run(mlp, l, B)
        if more:
            run(self_values, l + 1, A)
            run(project, l + 1, SELF, A)
        run(finish_mlp, l, B)
        if more:
            run(self_scores, l + 1, B)
            run(self_values, l + 1, B)

    for hf in range(2):
        with jax.named_scope('gwait'):
            gathers[(L - 1, MLP, hf)].wait()
        xfT[:, hf * LANES:(hf + 1) * LANES] = xng[L - 1, 1, hf].astype(F32).T.astype(BF)

    with jax.named_scope('headwait'):
        for i in range(len(starts)):
            for cp in head_copies(i):
                cp.wait()
    with jax.named_scope('head'):
        m, total = jnp.full((8, ROWS), -jnp.inf, F32), jnp.zeros((8, ROWS), F32)
        for i in range(len(starts) + 1):
            m2, more = m, total
            if i > 0:
                z = zout[starts[i - 1]:starts[i - 1] + sizes[i - 1], :].reshape(-1, 8, ROWS)
                more = total + jnp.sum(jnp.exp(z - m[None]), axis=0)
            if i < len(starts):
                z = dot(jnp.concatenate([mkb[i, 0:sizes[i]], mvb[i, 0:sizes[i]]], axis=1), xfT[...])
                zout[starts[i]:starts[i] + sizes[i], :] = z
                m2 = jnp.maximum(m, jnp.max(z.reshape(-1, 8, ROWS), axis=0))
                if i > 0:
                    more = more * jnp.exp(m - m2)
            m, total = m2, more
        s = total
    top = jnp.max(m, axis=0, keepdims=True)
    tot = jnp.sum(s * jnp.exp(m - top), axis=0, keepdims=True)
    msb[0:8] = jnp.broadcast_to(top, (8, ROWS))
    msb[8:16] = jnp.broadcast_to(tot, (8, ROWS))
    outs = [remote(msb, msr.at[i], ls.at[i], lr.at[i], dev) for i, dev in enumerate(others)]
    with jax.named_scope('lsewait'):
        for o in outs:
            o.wait()
    big = msb[0:8]
    for i in range(len(others)):
        big = jnp.maximum(big, msr[i, 0:8])
    total = msb[8:16] * jnp.exp(msb[0:8] - big)
    for i in range(len(others)):
        total = total + msr[i, 8:16] * jnp.exp(msr[i, 0:8] - big)
    lse_out[...] = big + jnp.log(total)


def decode(args):
    (tok, lens, kc, vc, mk, mv, lna, wqkv, bqkv, wo, bo, lnc, wqc, bqc, woc, boc, lnm, w1, b1, w2, b2, lnf, wout) = args
    L, ctx = kc.shape[:2]
    V = pltpu.VMEM
    dma = pltpu.SemaphoreType.DMA
    hbm = pl.BlockSpec(memory_space=pltpu.HBM)
    vm = pl.BlockSpec(memory_space=V)
    streamed = [kc, vc, mk, mv, wqkv, wo, wqc, woc, w1, w2, wout]
    return pl.pallas_call(
        decode_kernel,
        out_shape=(V((8, ROWS), F32), V((L, LANES, ROWS), BF), V((L, LANES, ROWS), BF),
                   V(kc.shape[1:], BF), V(kc.shape[1:], BF), V(vc.shape, BF), V((wout.shape[0], ROWS), F32)),
        in_specs=[hbm if any(a is b for b in streamed) else vm for a in args],
        out_specs=(vm,) * 7,
        scratch_shapes=[
            V((RING, CHUNK * LANES, ROWS), BF), V((RING, CHUNK * LANES, ROWS), BF),
            V((L, 3, WIDTH, LANES), BF), V((L, 2, 2, LANES, WIDTH), BF), V((L, WIDTH, LANES), BF),
            V((L, 2, WIDTH, WIDTH), BF), V((L, 2, WIDTH, WIDTH), BF), V((L, WIDTH), F32),
            V((2, HD, WIDTH), F32), V((L, 2, 2, LANES, WIDTH), BF), V((WIDTH, ROWS), BF),
            V((L, 2, 2, LANES, LANES), BF), V((L, 2, 2, HD, LANES), BF),
            V((L, 3, 2, HD, WIDTH), BF), V((L, 3, 2, HD, WIDTH), BF),
            V((2, LANES, LANES), F32), V((2, ROWS, LANES), BF), V((2 * (CHUNK - ON_VECTOR), (CHUNK - ON_VECTOR) * LANES), BF), V((32, ROWS), BF), V((LANES, ROWS), BF), V((2, HD, LANES), F32),
            V((LANES, LANES), F32), V((LANES, LANES), F32), V((LANES, LANES), F32), V((ctx * 2, LANES), F32), V((8, LANES), F32),
            V((16, ROWS), F32), V((3, 16, ROWS), F32),
            dma((L, 6)), dma((L, 5)), dma((L, 5)), dma((L, 4)), dma((RING,)), dma((RING,)),
            dma((L, 2, 2)), dma((L, 2, 2)), dma((L, 3, 2)), dma((L, 3, 2)), dma((L, 2, 2)), dma((L, 2, 2)), dma((3,)), dma((3,)),
        ],
        compiler_params=pltpu.CompilerParams(collective_id=0, has_side_effects=True, vmem_limit_bytes=DECODE_VMEM),
        name='decode',
    )(*args)


def write_kernel(lens, kn, vn, k0, k1, vc, z, lse, k_out, v_out, logp, kb, vb, zb, k_sem, v_sem, z_sem):
    L, ctx = vc.shape[:2]
    slots, blk = vb.shape[:2]
    per = ctx // blk
    steps = L * per
    vocab = z.shape[0]
    starts = list(range(0, vocab, Z_ROWS))

    def copies(i):
        slot, part = i % slots, pl.ds((i % per) * blk, blk)
        size = min(Z_ROWS, vocab - starts[i])
        return (pltpu.make_async_copy(kb.at[slot], k_out.at[i // per, part], k_sem.at[slot]),
                pltpu.make_async_copy(vb.at[slot], v_out.at[i // per, part], v_sem.at[slot]),
                pltpu.make_async_copy(zb.at[slot, pl.ds(0, size)], logp.at[pl.ds(starts[i], size)], z_sem.at[slot]))

    for i in range(steps):
        slot, l, first = i % slots, i // per, (i % per) * blk
        key_out, value_out, logp_out = copies(i)
        if i >= slots:
            for cp in copies(i - slots):
                cp.wait()

        def edit(b, src, new):
            def body(j, _):
                b[slot, j] = jnp.where(lens[...] == first + j, new[l], src[first + j])
                return 0
            lax.fori_loop(0, blk, body, 0)

        edit(kb, (k0, k1)[l], kn)
        key_out.start()
        edit(vb, vc.at[l], vn)
        value_out.start()
        size = min(Z_ROWS, vocab - starts[i])
        zb[slot, 0:size, :] = z[starts[i]:starts[i] + size, :] - lse[0:1]
        logp_out.start()
    for i in range(steps - slots, steps):
        for cp in copies(i):
            cp.wait()


def write_out(lens, kn, vn, ks, vc, z, lse):
    L, ctx = vc.shape[:2]
    V = pltpu.VMEM
    dma = pltpu.SemaphoreType.DMA
    slots, blk = 2, ctx // 4
    vm, hbm = pl.BlockSpec(memory_space=V), pl.BlockSpec(memory_space=pltpu.HBM)
    cache = V((slots, blk) + vc.shape[2:], BF)
    like = lambda a: jax.ShapeDtypeStruct(a.shape, a.dtype)
    return pl.pallas_call(
        write_kernel,
        out_shape=(like(vc), like(vc), like(z)),
        in_specs=[vm] * 8,
        out_specs=(hbm,) * 3,
        scratch_shapes=[cache, cache, V((slots, Z_ROWS, ROWS), F32), dma((slots,)), dma((slots,)), dma((slots,))],
        compiler_params=pltpu.CompilerParams(vmem_limit_bytes=WRITE_VMEM),
        name='write',
    )(lens, kn, vn, *ks, vc, z, lse)


def solution(mesh):
    cache_spec = P(None, 'dp', None, 'tp', None)
    in_specs = (P('dp', None), P('dp'), cache_spec, cache_spec, cache_spec, cache_spec,
                P(), P(None, None, None, 'tp'), P(None, None, 'tp'), P(None, 'tp', None), P(),
                P(), P(None, None, 'tp'), P(None, 'tp'), P(None, 'tp', None), P(),
                P(), P(None, None, 'tp'), P(None, 'tp'), P(None, 'tp', None), P(),
                P(), P(None, 'tp'))
    out_specs = (P('dp', 'tp'), cache_spec, cache_spec)

    def local_step(tokens, seq_lens, k_cache, v_cache, mem_k, mem_v, ln_attn, w_qkv, b_qkv, w_o, b_o, ln_cross, w_qc, b_qc, w_oc, b_oc, ln_mlp, w_fc1, b_fc1, w_fc2, b_fc2, ln_final, w_out):
        L, B, ctx, H, D = k_cache.shape
        M = mem_k.shape[2]
        lens = seq_lens.reshape(1, B)
        kc = k_cache.transpose(0, 2, 3, 4, 1).reshape(L, ctx, H * D, B)
        vc = v_cache.transpose(0, 2, 3, 4, 1).reshape(L, ctx, H * D, B)
        mk = mem_k.transpose(0, 1, 3, 4, 2).reshape(L, B * H * D, M)
        mv = mem_v.transpose(0, 1, 3, 4, 2).reshape(L, B * H * D, M)
        wout = w_out.T
        lse, kn, vn, k0, k1, held, z = decode((tokens, lens, kc, vc, mk, mv, ln_attn, w_qkv.transpose(0, 2, 1, 3), b_qkv.transpose(1, 0, 2), w_o, b_o, ln_cross, w_qc, b_qc,
                                  w_oc, b_oc, ln_mlp, w_fc1, b_fc1, w_fc2, b_fc2, ln_final, wout))
        k, v, logp = write_out(lens, kn, vn, (k0, k1), held, z, lse)
        back = lambda a: a.reshape(L, ctx, H, D, B).transpose(0, 4, 1, 2, 3)
        return logp.T, back(k), back(v)

    return jax.shard_map(local_step, mesh=mesh, in_specs=in_specs, out_specs=out_specs, check_vma=False)
```

```python
import functools
import math

import jax
import jax.numpy as jnp
from jax import lax
from jax.experimental import pallas as pl
from jax.experimental.pallas import tpu as pltpu
from jax.sharding import PartitionSpec as P

BF = jnp.bfloat16
F32 = jnp.float32
MESH = pl.DeviceIdType.MESH
RING = 8
CHUNK = 16
ON_VECTOR = 8
HEAD_ROWS = 2048
Z_ROWS = 1552
DECODE_VMEM = 30 << 20
WRITE_VMEM = 12 << 20
LANES = 128
HD = 64
ROWS = 256
WIDTH = 512
SELF, CROSS, MLP = range(3)
A, B = range(2)


def dot(a, b):
    return jnp.dot(a, b, preferred_element_type=F32)


def dot_nt(a, b):
    return lax.dot_general(a, b, (((1,), (1,)), ((), ())), preferred_element_type=F32)


def norm(x, gain, shift):
    mean = jnp.mean(x, axis=-1, keepdims=True)
    centred = x - mean
    var = jnp.mean(centred * centred, axis=-1, keepdims=True)
    return (centred * lax.rsqrt(var + 1e-5) * gain + shift).astype(BF)


def iota(shape, dim):
    return lax.broadcasted_iota(jnp.int32, shape, dim)


def fold(x8, op):
    x8 = op(x8, pltpu.roll(x8, 4, 0))
    return op(x8, pltpu.roll(x8, 2, 0))


def decode_kernel(small, tok, lens, kc, vc, mk, mv, lna, wqkv, bqkv, wo, bo, lnc, wqc, bqc, woc, boc, lnm, w1, b1, w2, b2, lnf, wout,
                  lse_out, kn_out, vn_out, ck0, ck1, cvb, zout,
                  mkb, mvb, wqkvb, wob, wqcb, w1b, w2b, b1x,
                  xown, xng, xfT, obuf, orecv, xsend, xrecv, qTc, q2s, qbm, pcar, pm, racc, qT, kT, vT, ss, pns, msb, msr,
                  lw_sem, rws_sem, rwr_sem, c_sem, mk_sem, mv_sem, es, er, xs, xr, gs, gr, ls, lr):
    L = kc.shape[0]
    ctx = kc.shape[1]
    split = ctx // 8 * 4 + 4
    me = lax.axis_index('tp')
    c = lax.rem(me, 2)
    partner = me + 1 - 2 * c
    peer = lax.rem(me + 2, 4)
    own = pl.multiple_of(c * HD, HD)
    oth = pl.multiple_of((1 - c) * HD, HD)

    def seq_chunk(n):
        layer = n // 16
        within = n % 16
        half = within // 8
        sub = (within % 8) // 4
        grp = sub + (1 - 2 * sub) * (1 - c)
        seq = half * LANES + grp * HD + (within % 4) * CHUNK
        return layer, seq

    def mem_copy(n, src, dst, sem):
        layer, seq = seq_chunk(n)
        slot = lax.rem(n, RING)
        return pltpu.make_async_copy(src.at[layer, pl.ds(seq * LANES, CHUNK * LANES)], dst.at[slot], sem.at[slot])

    def key_copy(n):
        return mem_copy(n, mk, mkb, mk_sem)

    def value_copy(n):
        return mem_copy(n, mv, mvb, mv_sem)

    def refill(copy, n):
        @pl.when(n + RING < 16 * L)
        def _():
            copy(n + RING).start()

    def cache_copies(l):
        def piece(src, dst, i, start, size):
            part = pl.ds(start, size)
            dst = dst.at[l, part] if dst is cvb else dst[l].at[part]
            return pltpu.make_async_copy(src.at[l, part], dst, c_sem.at[l, i])
        return [[piece(src, dst, 2 * i + p, p * split, (split, ctx - split)[p]) for p in range(2)]
                for i, (src, dst) in enumerate(((kc, (ck0, ck1)), (vc, cvb)))]

    def weight_copies(l):
        pairs = ((wqkv.at[l], wqkvb.at[l]), (wo.at[l], wob.at[l, 0, 0]), (wqc.at[l], wqcb.at[l]),
                 (woc.at[l], wob.at[l, 1, 0]), (w1.at[l], w1b.at[l, 0]), (w2.at[l], w2b.at[l, 0]))
        return [pltpu.make_async_copy(s, d, lw_sem.at[l, i]) for i, (s, d) in enumerate(pairs)]

    def shared_copies(l):
        pairs = [(wo.at[l], wob.at[l, 0, 1]), (woc.at[l], wob.at[l, 1, 1]), (w1.at[l], w1b.at[l, 1]), (w2.at[l], w2b.at[l, 1])]
        if l == 0:
            pairs.append((b1, b1x))
        return [pltpu.make_async_remote_copy(s, d, rws_sem.at[l, i], rwr_sem.at[l, i], device_id={'tp': partner}, device_id_type=MESH)
                for i, (s, d) in enumerate(pairs)]

    vocab = wout.shape[0]
    starts = list(range(0, vocab, HEAD_ROWS))
    sizes = [min(HEAD_ROWS, vocab - first) for first in starts]

    def head_copies(i):
        rows = pl.ds(starts[i], sizes[i])
        return [pltpu.make_async_copy(wout.at[rows, pl.ds(t * ROWS, ROWS)], dst.at[i, pl.ds(0, sizes[i])], sem.at[i])
                for t, (dst, sem) in enumerate(((mkb, mk_sem), (mvb, mv_sem)))]

    weights = [weight_copies(l) for l in range(L)]
    shared = [shared_copies(l) for l in range(L)]
    caches = [cache_copies(l) for l in range(L)]

    for cp in small:
        cp.start()
    weights[A][SELF].start()
    caches[A][0][0].start()
    barrier = pltpu.get_barrier_semaphore()
    others = [lax.rem(me + d, 4) for d in range(1, 4)]
    for dev in others:
        pl.semaphore_signal(barrier, inc=1, device_id={'tp': dev}, device_id_type=MESH)

    def meet():
        with jax.named_scope('barrier'):
            pl.semaphore_wait(barrier, len(others))
        shared[A][SELF].start()
        for w in weights[A][1:]:
            w.start()

    def fetch_memory():
        for n in range(RING):
            key_copy(n).start()
            value_copy(n).start()

    def share(l):
        for cp in shared[l][1 - l:]:
            cp.start()

    def prepare():
        pm[...] = jnp.zeros_like(pm)
        qbm[...] = jnp.where(iota(qbm.shape, 1) // HD == iota(qbm.shape, 0), 1.0, 0.0).astype(BF)
        for h in range(2):
            xown[h] = tok[pl.ds(pl.multiple_of(h * LANES + own, HD), HD), :].astype(F32)

    def fetch_caches(l):
        for cp in (caches[l][0] + caches[l][1])[1 - l:]:
            cp.start()

    def self_scores(l, hf):
        lanes = pl.ds(hf * LANES, LANES)
        if l == 0:
            if hf == A:
                for cp in small:
                    cp.wait()
            xn = norm(tok[hf * LANES:(hf + 1) * LANES, :].astype(F32), lna[l, 0:1], lna[l, 1:2])
            if hf == A:
                fetch_caches(l)
        else:
            with jax.named_scope('gwait'):
                gathers[(l - 1, MLP, hf)].wait()
            xn = xng[l - 1, 1, hf]
        if hf == A:
            weights[l][SELF].wait()
        for i, ref in enumerate((qT, kT, vT)):
            y = (dot(xn, wqkvb[l, i]) + bqkv[i, l:l + 1]).astype(BF)
            ref[...] = y.astype(F32).T
        kn_out[l, :, lanes] = kT[...].astype(BF)
        vn_out[l, :, lanes] = vT[...].astype(BF)

        def k_body(t, _):
            blk = (ck0, ck1)[l][pl.ds(t * 4, 4), :, lanes].astype(F32) * qT[...][None]
            ss[pl.ds(pl.multiple_of(t * 8, 8), 8), :] = jnp.sum(blk.reshape(8, HD, LANES), axis=1) * 0.125
            return 0

        for p in range(2):
            if hf == A:
                with jax.named_scope('kcwait'):
                    caches[l][0][p].wait()
            lax.fori_loop((0, split // 4)[p], (split // 4, ctx // 4)[p], k_body, 0)
        snew = jnp.sum((qT[...] * kT[...]).reshape(2, HD, LANES), axis=1) * 0.125
        snew = jnp.concatenate([snew] * 4, axis=0)
        s = ss[...].reshape(ctx // 4, 8, LANES)
        pos = iota(s.shape, 0) * 4 + iota(s.shape, 1) // 2
        ln = lens[0:1, lanes][None]
        fresh = pos == ln
        s = jnp.where(fresh, snew[None], jnp.where(pos < ln, s, -1e30))
        m8 = fold(jnp.max(s, axis=0), jnp.maximum)
        p = jnp.exp(s - m8[None])
        l8 = fold(jnp.sum(p, axis=0), jnp.add)
        p = (p / l8[None]).astype(BF).astype(F32)
        pns[...] = fold(jnp.sum(jnp.where(fresh, p, 0.0), axis=0), jnp.add)
        ss[...] = jnp.where(fresh, 0.0, p).reshape(ctx * 2, LANES)

    def self_values(l, hf):
        lanes = pl.ds(hf * LANES, LANES)

        def v_body(t, acc):
            blk = cvb[l, pl.ds(t * 4, 4), :, lanes].astype(F32)
            pr = ss[pl.ds(pl.multiple_of(t * 8, 8), 8), :]
            acc = list(acc)
            for j in range(4):
                for h in range(2):
                    acc[h] = acc[h] + blk[j, h * HD:(h + 1) * HD] * pr[2 * j + h:2 * j + h + 1]
            return tuple(acc)

        acc = tuple(vT[h * HD:(h + 1) * HD, :] * pns[h:h + 1] for h in range(2))
        for p in range(2):
            if hf == A:
                with jax.named_scope('vcwait'):
                    caches[l][1][p].wait()
            acc = lax.fori_loop((0, split // 4)[p], (split // 4, ctx // 4)[p], v_body, acc)
        oT = jnp.concatenate(acc, axis=0).astype(BF).astype(F32)
        obuf[l, SELF, hf] = oT.T.astype(BF)
        send_o(l, SELF, hf)

    swaps, crosses, gathers = {}, {}, {}

    def remote(src, dst, ssem, rsem, dev):
        cp = pltpu.make_async_remote_copy(src, dst, ssem, rsem, device_id={'tp': dev}, device_id_type=MESH)
        cp.start()
        return cp

    def send_o(l, k, hf):
        swaps[(l, k, hf)] = remote(obuf.at[l, k, hf, pl.ds(oth, HD)], orecv.at[l, k, hf], es.at[l, k, hf], er.at[l, k, hf], partner)

    def send_x(l, k, hf, part):
        xsend[l, k, hf] = part.astype(BF)
        crosses[(l, k, hf)] = remote(xsend.at[l, k, hf], xrecv.at[l, k, hf], xs.at[l, k, hf], xr.at[l, k, hf], peer)

    def project(l, k, hf):
        if hf == 0:
            weights[l][2 * k + 1].wait()
            shared[l][k].wait()
        with jax.named_scope('owait'):
            swaps[(l, k, hf)].wait()
        part = dot(obuf[l, k, hf, pl.ds(own, HD)], wob[l, k, 0]) + dot(orecv[l, k, hf], wob[l, k, 1])
        send_x(l, k, hf, part)

    def add_up(l, k, hf, bias):
        with jax.named_scope('xwait'):
            crosses[(l, k, hf)].wait()
        x = xown[hf] + (xsend[l, k, hf].astype(F32) + xrecv[l, k, hf].astype(F32)) + bias
        xown[hf] = x
        return x

    def gather(l, k, hf, xn):
        rows = pl.ds(own, HD)
        ref = xng.at[l, k // 2, hf, rows]
        xng[l, k // 2, hf, rows] = xn
        gathers[(l, k, hf)] = remote(ref, ref, gs.at[l, k // 2, hf], gr.at[l, k // 2, hf], partner)

    def finish_self(l, hf):
        x = add_up(l, SELF, hf, bo[l:l + 1])
        gather(l, SELF, hf, norm(x, lnc[l, 0:1], lnc[l, 1:2]))

    def scores(n, shift, hf):
        with jax.named_scope('memwait'):
            key_copy(n).wait()
        slot = lax.rem(n, RING)
        qc = pltpu.roll(qTc[hf], lax.rem(2 * LANES - shift, LANES), 1)
        rows = []
        for i in range(ON_VECTOR):
            q = jnp.broadcast_to(qc[:, i:i + 1], (LANES, LANES))
            halves = []
            for t in range(2):
                part = mkb[slot, i * LANES:(i + 1) * LANES, t * LANES:(t + 1) * LANES].astype(F32) * q
                halves.append(jnp.sum(part.reshape(2, HD, LANES), axis=1))
            rows.append(jnp.concatenate(halves, axis=1))
        rest = CHUNK - ON_VECTOR
        q2 = q2s[hf, pl.ds(pl.multiple_of(2 * shift + 2 * ON_VECTOR, 16), 2 * rest), :]
        qbd = jnp.concatenate([q2] * rest, axis=1) * qbm[...]
        rows.append(dot(qbd, mkb[slot, ON_VECTOR * LANES:CHUNK * LANES]))
        s = jnp.concatenate(rows, axis=0) * 0.125
        e = jnp.exp(s - jnp.max(s, axis=-1, keepdims=True))
        return (e / jnp.sum(e, axis=-1, keepdims=True)).astype(BF)

    def values(n, t, p):
        slot = lax.rem(n, RING)
        pm[pl.ds(pl.multiple_of(t * 32, 32), 32), :] = p
        lane = iota((HD, LANES), 1)
        r = [racc[h] for h in range(2)]
        for part in range(2):
            seqs = CHUNK // 2
            out = dot_nt(mvb[slot, part * seqs * LANES:(part + 1) * seqs * LANES], pm[...])
            for i in range(seqs):
                for h in range(2):
                    first = i * LANES + h * HD
                    r[h] = jnp.where(lane == t * 32 + 2 * (part * seqs + i) + h, out[first:first + HD], r[h])
        for h in range(2):
            racc[h] = r[h]

    def base_of(l, hf, sub):
        return l * 16 + hf * 8 + sub * 4, (sub + (1 - 2 * sub) * (1 - c)) * HD

    def start_cross(l, hf):
        if hf == A:
            weights[l][2].wait()
        with jax.named_scope('gwait'):
            gathers[(l, SELF, hf)].wait()
        q = (dot(xng[l, SELF, hf], wqcb[l]) + bqc[l:l + 1]).astype(BF)
        qTc[hf] = q.astype(F32).T
        twice = jnp.where(iota((ROWS, LANES), 0) // 2 == iota((ROWS, LANES), 1), 1.0, 0.0).astype(BF)
        q2s[hf] = dot(twice, q).astype(BF)
        n, seq = base_of(l, hf, 0)
        pcar[...] = scores(n, seq, hf)
        refill(key_copy, n)

    def cross_part(l, hf, sub):
        base, seq = base_of(l, hf, sub)
        last = sub == 1

        def body(t, p):
            n = base + t
            value_copy(n).wait()
            if last:
                shift = seq + (t + 1) * CHUNK
            else:
                shift = jnp.where(t == 3, base_of(l, hf, 1)[1], seq + (t + 1) * CHUNK)
            after = scores(n + 1, shift, hf)
            values(n, t, p)
            refill(key_copy, n + 1)
            refill(value_copy, n)
            return after

        p = lax.fori_loop(0, 3 if last else 4, body, pcar[...])
        if last:
            value_copy(base + 3).wait()
            values(base + 3, 3, p)
            refill(value_copy, base + 3)
        else:
            pcar[...] = p
        lane = iota((LANES, LANES), 1)
        r = jnp.concatenate([racc[0], racc[1]], axis=0)
        r = jnp.where(lax.rem(lane, 2) == iota((LANES, LANES), 0) // HD, r, 0.0).astype(BF)
        sel = jnp.where(iota((HD, LANES), 1) // 2 == iota((HD, LANES), 0), 1.0, 0.0).astype(BF)
        obuf[l, CROSS, hf, pl.ds(pl.multiple_of(seq, HD), HD)] = dot_nt(sel, r).astype(BF)
        if not last:
            send_o(l, CROSS, hf)

    def mlp(l, hf):
        x = add_up(l, CROSS, hf, boc[l:l + 1])
        xn = norm(x, lnm[l, 0:1], lnm[l, 1:2])
        if hf == 0:
            weights[l][4].wait()
            weights[l][5].wait()
            shared[l][2].wait()
            shared[l][3].wait()
            if l == 0:
                shared[0][4].wait()
        part = None
        for k in range(2):
            a = dot(xn, w1b[l, k]) + (b1 if k == 0 else b1x)[l:l + 1]
            a = (0.5 * a * (1.0 + lax.erf(a * math.sqrt(0.5)))).astype(BF)
            d = dot(a, w2b[l, k])
            part = d if part is None else part + d
        send_x(l, MLP, hf, part)

    def finish_mlp(l, hf):
        x = add_up(l, MLP, hf, b2[l:l + 1])
        last = l == L - 1
        params = lnf if last else lna.at[l + 1]
        gather(l, MLP, hf, norm(x, params[0:1], params[1:2]))

    def run(step, *args):
        with jax.named_scope(step.__name__ + '_' + '_'.join(str(a) for a in args)):
            step(*args)

    run(self_scores, A, A)
    run(meet)
    run(self_values, A, A)
    fetch_memory()
    run(self_scores, A, B)
    run(project, A, SELF, A)
    run(self_values, A, B)
    run(prepare)
    run(project, A, SELF, B)
    for l in range(L):
        more = l + 1 < L
        if l == 0:
            run(finish_self, l, A)
        run(start_cross, l, A)
        if l > 0:
            run(project, l, SELF, B)
        if l == 0:
            share(A)
        run(cross_part, l, A, 0)
        run(finish_self, l, B)
        if l == 0:
            for w in weights[B]:
                w.start()
            fetch_caches(B)
        run(cross_part, l, A, 1)
        run(project, l, CROSS, A)
        run(start_cross, l, B)
        if l == 0:
            share(B)
        run(cross_part, l, B, 0)
        run(mlp, l, A)
        run(cross_part, l, B, 1)
        if not more:
            for i in range(len(starts)):
                for cp in head_copies(i):
                    cp.start()
        run(project, l, CROSS, B)
        run(finish_mlp, l, A)
        if more:
            run(self_scores, l + 1, A)
        run(mlp, l, B)
        if more:
            run(self_values, l + 1, A)
            run(project, l + 1, SELF, A)
        run(finish_mlp, l, B)
        if more:
            run(self_scores, l + 1, B)
            run(finish_self, l + 1, A)
            run(self_values, l + 1, B)

    for hf in range(2):
        with jax.named_scope('gwait'):
            gathers[(L - 1, MLP, hf)].wait()
        xfT[:, hf * LANES:(hf + 1) * LANES] = xng[L - 1, 1, hf].astype(F32).T.astype(BF)

    with jax.named_scope('headwait'):
        for i in range(len(starts)):
            for cp in head_copies(i):
                cp.wait()
    with jax.named_scope('head'):
        m, total = jnp.full((8, ROWS), -jnp.inf, F32), jnp.zeros((8, ROWS), F32)
        for i in range(len(starts) + 1):
            m2, more = m, total
            if i > 0:
                z = zout[starts[i - 1]:starts[i - 1] + sizes[i - 1], :].reshape(-1, 8, ROWS)
                more = total + jnp.sum(jnp.exp(z - m[None]), axis=0)
            if i < len(starts):
                z = dot(jnp.concatenate([mkb[i, 0:sizes[i]], mvb[i, 0:sizes[i]]], axis=1), xfT[...])
                zout[starts[i]:starts[i] + sizes[i], :] = z
                m2 = jnp.maximum(m, jnp.max(z.reshape(-1, 8, ROWS), axis=0))
                if i > 0:
                    more = more * jnp.exp(m - m2)
            m, total = m2, more
        s = total
    top = jnp.max(m, axis=0, keepdims=True)
    tot = jnp.sum(s * jnp.exp(m - top), axis=0, keepdims=True)
    msb[0:8] = jnp.broadcast_to(top, (8, ROWS))
    msb[8:16] = jnp.broadcast_to(tot, (8, ROWS))
    outs = [remote(msb, msr.at[i], ls.at[i], lr.at[i], dev) for i, dev in enumerate(others)]
    with jax.named_scope('lsewait'):
        for o in outs:
            o.wait()
    big = msb[0:8]
    for i in range(len(others)):
        big = jnp.maximum(big, msr[i, 0:8])
    total = msb[8:16] * jnp.exp(msb[0:8] - big)
    for i in range(len(others)):
        total = total + msr[i, 8:16] * jnp.exp(msr[i, 0:8] - big)
    lse_out[...] = big + jnp.log(total)


def decode_entry(streamed, *refs):
    n_in = len(streamed)
    ins, rest = list(refs[:n_in]), refs[n_in:]
    small = [i for i in range(n_in) if not streamed[i]]
    held, sem = rest[-len(small) - 1:-1], rest[-1]
    copies = []
    for k, i in enumerate(small):
        copies.append(pltpu.make_async_copy(ins[i], held[k], sem.at[k]))
        ins[i] = held[k]
    decode_kernel(copies, *ins, *rest[:-len(small) - 1])


def decode(args):
    (tok, lens, kc, vc, mk, mv, lna, wqkv, bqkv, wo, bo, lnc, wqc, bqc, woc, boc, lnm, w1, b1, w2, b2, lnf, wout) = args
    L, ctx = kc.shape[:2]
    V = pltpu.VMEM
    dma = pltpu.SemaphoreType.DMA
    hbm = pl.BlockSpec(memory_space=pltpu.HBM)
    vm = pl.BlockSpec(memory_space=V)
    streamed = [kc, vc, mk, mv, wqkv, wo, wqc, woc, w1, w2, wout]
    flags = [any(a is b for b in streamed) for a in args]
    small = [a for a, f in zip(args, flags) if not f]
    return pl.pallas_call(
        functools.partial(decode_entry, flags),
        out_shape=(V((8, ROWS), F32), V((L, LANES, ROWS), BF), V((L, LANES, ROWS), BF),
                   V(kc.shape[1:], BF), V(kc.shape[1:], BF), V(vc.shape, BF), V((wout.shape[0], ROWS), F32)),
        in_specs=[hbm] * len(args),
        out_specs=(vm,) * 7,
        scratch_shapes=[
            V((RING, CHUNK * LANES, ROWS), BF), V((RING, CHUNK * LANES, ROWS), BF),
            V((L, 3, WIDTH, LANES), BF), V((L, 2, 2, LANES, WIDTH), BF), V((L, WIDTH, LANES), BF),
            V((L, 2, WIDTH, WIDTH), BF), V((L, 2, WIDTH, WIDTH), BF), V((L, WIDTH), F32),
            V((2, HD, WIDTH), F32), V((L, 2, 2, LANES, WIDTH), BF), V((WIDTH, ROWS), BF),
            V((L, 2, 2, LANES, LANES), BF), V((L, 2, 2, HD, LANES), BF),
            V((L, 3, 2, HD, WIDTH), BF), V((L, 3, 2, HD, WIDTH), BF),
            V((2, LANES, LANES), F32), V((2, ROWS, LANES), BF), V((2 * (CHUNK - ON_VECTOR), (CHUNK - ON_VECTOR) * LANES), BF), V((32, ROWS), BF), V((LANES, ROWS), BF), V((2, HD, LANES), F32),
            V((LANES, LANES), F32), V((LANES, LANES), F32), V((LANES, LANES), F32), V((ctx * 2, LANES), F32), V((8, LANES), F32),
            V((16, ROWS), F32), V((3, 16, ROWS), F32),
            dma((L, 6)), dma((L, 5)), dma((L, 5)), dma((L, 4)), dma((RING,)), dma((RING,)),
            dma((L, 2, 2)), dma((L, 2, 2)), dma((L, 3, 2)), dma((L, 3, 2)), dma((L, 2, 2)), dma((L, 2, 2)), dma((3,)), dma((3,)),
        ] + [V(a.shape, a.dtype) for a in small] + [dma((len(small),))],
        compiler_params=pltpu.CompilerParams(collective_id=0, has_side_effects=True, vmem_limit_bytes=DECODE_VMEM),
        name='decode',
    )(*args)


def write_kernel(lens, kn, vn, k0, k1, vc, z, lse, k_out, v_out, logp, kb, vb, zb, k_sem, v_sem, z_sem):
    L, ctx = vc.shape[:2]
    slots, blk = vb.shape[:2]
    per = ctx // blk
    steps = L * per
    vocab = z.shape[0]
    starts = list(range(0, vocab, Z_ROWS))

    def copies(i):
        slot, part = i % slots, pl.ds((i % per) * blk, blk)
        size = min(Z_ROWS, vocab - starts[i])
        return (pltpu.make_async_copy(kb.at[slot], k_out.at[i // per, part], k_sem.at[slot]),
                pltpu.make_async_copy(vb.at[slot], v_out.at[i // per, part], v_sem.at[slot]),
                pltpu.make_async_copy(zb.at[slot, pl.ds(0, size)], logp.at[pl.ds(starts[i], size)], z_sem.at[slot]))

    for i in range(steps):
        slot, l, first = i % slots, i // per, (i % per) * blk
        key_out, value_out, logp_out = copies(i)
        if i >= slots:
            for cp in copies(i - slots):
                cp.wait()

        def edit(b, src, new):
            def body(j, _):
                b[slot, j] = jnp.where(lens[...] == first + j, new[l], src[first + j])
                return 0
            lax.fori_loop(0, blk, body, 0)

        edit(kb, (k0, k1)[l], kn)
        key_out.start()
        edit(vb, vc.at[l], vn)
        value_out.start()
        size = min(Z_ROWS, vocab - starts[i])
        zb[slot, 0:size, :] = z[starts[i]:starts[i] + size, :] - lse[0:1]
        logp_out.start()
    for i in range(steps - slots, steps):
        for cp in copies(i):
            cp.wait()


def write_out(lens, kn, vn, ks, vc, z, lse):
    L, ctx = vc.shape[:2]
    V = pltpu.VMEM
    dma = pltpu.SemaphoreType.DMA
    slots, blk = 2, ctx // 4
    vm, hbm = pl.BlockSpec(memory_space=V), pl.BlockSpec(memory_space=pltpu.HBM)
    cache = V((slots, blk) + vc.shape[2:], BF)
    like = lambda a: jax.ShapeDtypeStruct(a.shape, a.dtype)
    return pl.pallas_call(
        write_kernel,
        out_shape=(like(vc), like(vc), like(z)),
        in_specs=[vm] * 8,
        out_specs=(hbm,) * 3,
        scratch_shapes=[cache, cache, V((slots, Z_ROWS, ROWS), F32), dma((slots,)), dma((slots,)), dma((slots,))],
        compiler_params=pltpu.CompilerParams(vmem_limit_bytes=WRITE_VMEM),
        name='write',
    )(lens, kn, vn, *ks, vc, z, lse)


def solution(mesh):
    cache_spec = P(None, 'dp', None, 'tp', None)
    in_specs = (P('dp', None), P('dp'), cache_spec, cache_spec, cache_spec, cache_spec,
                P(), P(None, None, None, 'tp'), P(None, None, 'tp'), P(None, 'tp', None), P(),
                P(), P(None, None, 'tp'), P(None, 'tp'), P(None, 'tp', None), P(),
                P(), P(None, None, 'tp'), P(None, 'tp'), P(None, 'tp', None), P(),
                P(), P(None, 'tp'))
    out_specs = (P('dp', 'tp'), cache_spec, cache_spec)

    def local_step(tokens, seq_lens, k_cache, v_cache, mem_k, mem_v, ln_attn, w_qkv, b_qkv, w_o, b_o, ln_cross, w_qc, b_qc, w_oc, b_oc, ln_mlp, w_fc1, b_fc1, w_fc2, b_fc2, ln_final, w_out):
        L, B, ctx, H, D = k_cache.shape
        M = mem_k.shape[2]
        lens = seq_lens.reshape(1, B)
        kc = k_cache.transpose(0, 2, 3, 4, 1).reshape(L, ctx, H * D, B)
        vc = v_cache.transpose(0, 2, 3, 4, 1).reshape(L, ctx, H * D, B)
        mk = mem_k.transpose(0, 1, 3, 4, 2).reshape(L, B * H * D, M)
        mv = mem_v.transpose(0, 1, 3, 4, 2).reshape(L, B * H * D, M)
        wout = w_out.T
        lse, kn, vn, k0, k1, held, z = decode((tokens, lens, kc, vc, mk, mv, ln_attn, w_qkv.transpose(0, 2, 1, 3), b_qkv.transpose(1, 0, 2), w_o, b_o, ln_cross, w_qc, b_qc,
                                  w_oc, b_oc, ln_mlp, w_fc1, b_fc1, w_fc2, b_fc2, ln_final, wout))
        k, v, logp = write_out(lens, kn, vn, (k0, k1), held, z, lse)
        back = lambda a: a.reshape(L, ctx, H, D, B).transpose(0, 4, 1, 2, 3)
        return logp.T, back(k), back(v)

    return jax.shard_map(local_step, mesh=mesh, in_specs=in_specs, out_specs=out_specs, check_vma=False)
```
